32 devices in a mesh: tile: 8 (over z, x), sub: 4 (over y, core).
Axes of the slice: x: 2, y: 2, z: 4, core: 2. Of those that a mesh axis runs over, the one named last changes fastest.
Arguments:
- initial_state: float32 [8, 64, 1024], P('tile', None, 'sub'), may hold values from -6 to 6
- cotangent: float32 [8, 64, 1024], P('tile', None, 'sub'), may hold values from -6 to 6
- w_in: bfloat16 [576, 1024], replicated, may hold values from -0.25 to 0.25
- b_in: float32 [1024], replicated, may hold values from -3 to 3
- w_out: bfloat16 [64, 1024], replicated, may hold values from -0.1875 to 0.1875
- edge_flips: int32 [8, 2], P('tile'), may hold values 0 or 1
Outputs:
- final_state: float32 [8, 64, 1024], P('tile', None, 'sub')
- grad_state: float32 [8, 64, 1024], P('tile', None, 'sub')
- grad_w_in: float32 [576, 1024], replicated
- grad_b_in: float32 [1024], replicated
- grad_w_out: float32 [64, 1024], replicated
The draws below stay inside these ranges and needn't reach their ends.
All inputs are finite; a program needn't handle non-finite values. No bound on the sum of `edge_flips` on one device may be relied on, other than what follows from the above.
Results may differ from the reference program's by a relative error of at most 0.006.
Values may be sent and summed in bfloat16 or wider, within the bound.
A program may use at most 64 MiB of HBM per device.

```python
import jax
import jax.numpy as jnp

LEVELS = 64
HIDDEN_SIZE = 1024
IN_WIDTH = 576
STEPS = 4
TILE_ROW = 4
SIDE = 32
COLS = 1024
TILES = 8


def set_ends(values, rng, low, high):
    shape = values.shape
    place = [jax.random.randint(jax.random.fold_in(rng, axis), (), 0, shape[axis]) for axis in range(len(shape))]
    values = values.at[tuple(place)].set(low)
    longest = shape.index(max(shape))
    place[longest] = (place[longest] + 1) % shape[longest]
    return values.at[tuple(place)].set(high)


def block_levels(stream_key, dims, split, least, largest):
    level, own = 1.0, jax.random.fold_in(stream_key, 6)
    for dim, shards_of in split:
        steps = jnp.exp(jax.random.uniform(jax.random.fold_in(own, dim), (shards_of,), jnp.float32, least / len(split), largest / len(split)))
        level = level * jnp.repeat(steps, dims[dim] // shards_of).reshape([-1 if axis == dim else 1 for axis in range(len(dims))])
    return level


def bell_draw(own_key, extent, deviation, bound, cuts=(), dtype=jnp.bfloat16):
    drawn = deviation * jax.random.normal(own_key, extent, jnp.float32)
    if cuts:
        drawn = drawn * block_levels(own_key, extent, cuts, -0.22, 0.18)
    return jnp.clip(drawn, -bound, bound).astype(dtype)


def setup_inputs(seed: int = 0) -> dict:
    key_list = jax.random.split(jax.random.key(seed), 7)
    return {
        "initial_state": bell_draw(key_list[0], (TILES, LEVELS, COLS), 1.0, 6.0, ((0, 8), (2, 4)), jnp.float32),
        "cotangent": bell_draw(key_list[1], (TILES, LEVELS, COLS), 1.0, 6.0, ((0, 8), (2, 4)), jnp.float32),
        "w_in": bell_draw(key_list[2], (IN_WIDTH, HIDDEN_SIZE), IN_WIDTH ** -0.5, 0.25),
        "b_in": bell_draw(key_list[3], (HIDDEN_SIZE,), 0.5, 3.0, (), jnp.float32),
        "w_out": bell_draw(key_list[4], (LEVELS, HIDDEN_SIZE), HIDDEN_SIZE ** -0.5, 0.1875),
        "edge_flips": set_ends((jax.random.randint(key_list[5], (TILES, 2), 0, 2) < 1).astype(jnp.int32), jax.random.fold_in(key_list[5], 1), 0, 1),
    }


STEP_SIZE = 0.25


def pad_tiles(current, edge_flips):
    west_col = jnp.roll(current[..., SIDE - 1:], 1, axis=0)
    east_col = jnp.roll(current[..., :1], -1, axis=0)
    extended = jnp.concatenate([west_col, current, east_col], axis=3)
    north_row = jnp.roll(extended[:, :, SIDE - 1, :], TILE_ROW, axis=0)
    south_row = jnp.roll(extended[:, :, 0, :], -TILE_ROW, axis=0)
    north_row = jnp.where(edge_flips[:, 0][:, None, None] == 1, north_row[..., ::-1], north_row)
    south_row = jnp.where(edge_flips[:, 1][:, None, None] == 1, south_row[..., ::-1], south_row)
    return jnp.concatenate([north_row[:, :, None], extended, south_row[:, :, None]], axis=2)


def unpad_tiles(pad_grad, edge_flips):
    extended = pad_grad[:, :, 1:-1, :]
    north_grad = pad_grad[:, :, 0, :]
    south_grad = pad_grad[:, :, -1, :]
    north_grad = jnp.where(edge_flips[:, 0][:, None, None] == 1, north_grad[..., ::-1], north_grad)
    south_grad = jnp.where(edge_flips[:, 1][:, None, None] == 1, south_grad[..., ::-1], south_grad)
    extended = extended.at[:, :, SIDE - 1, :].add(jnp.roll(north_grad, -TILE_ROW, axis=0))
    extended = extended.at[:, :, 0, :].add(jnp.roll(south_grad, TILE_ROW, axis=0))
    inner = extended[..., 1:-1]
    inner = inner.at[..., SIDE - 1].add(jnp.roll(extended[..., 0], -1, axis=0))
    inner = inner.at[..., 0].add(jnp.roll(extended[..., -1], 1, axis=0))
    return inner


def gather_patches(padded):
    pieces = [padded[:, :, row_shift:row_shift + SIDE, col_shift:col_shift + SIDE]
              for row_shift in range(3) for col_shift in range(3)]
    return jnp.stack(pieces, axis=1).reshape(TILES, 9 * LEVELS, COLS)


def scatter_patches(patch_grad):
    pieces = patch_grad.reshape(TILES, 9, LEVELS, SIDE, SIDE)
    total = jnp.zeros((TILES, LEVELS, SIDE + 2, SIDE + 2), jnp.float32)
    for row_shift in range(3):
        for col_shift in range(3):
            total = total + jnp.pad(pieces[:, 3 * row_shift + col_shift],
                                    ((0, 0), (0, 0), (row_shift, 2 - row_shift), (col_shift, 2 - col_shift)))
    return total


def reference(initial_state, cotangent, w_in, b_in, w_out, edge_flips):
    w_in32 = w_in.astype(jnp.float32)
    w_out32 = w_out.astype(jnp.float32)
    current = initial_state.reshape(TILES, LEVELS, SIDE, SIDE)
    saved_fields = []
    for step_index in range(STEPS):
        saved_fields.append(current)
        patch_vals = gather_patches(pad_tiles(current, edge_flips)).astype(jnp.bfloat16)
        pre_act = jnp.einsum('ih,nic->nhc', w_in32, patch_vals.astype(jnp.float32)) + b_in[None, :, None]
        hidden_vals = jax.nn.silu(pre_act).astype(jnp.bfloat16)
        tendency = jnp.einsum('lh,nhc->nlc', w_out32, hidden_vals.astype(jnp.float32))
        level_mean = jnp.sum(tendency, axis=(0, 2)) / (TILES * COLS)
        current = current + (STEP_SIZE * (tendency - level_mean[None, :, None])).reshape(current.shape)
    final_state = current.reshape(TILES, LEVELS, COLS)
    gradient = cotangent
    grad_w_in = jnp.zeros((IN_WIDTH, HIDDEN_SIZE), jnp.float32)
    grad_w_out = jnp.zeros((LEVELS, HIDDEN_SIZE), jnp.float32)
    grad_b_in = jnp.zeros((HIDDEN_SIZE,), jnp.float32)
    for step_index in reversed(range(STEPS)):
        patch_vals = gather_patches(pad_tiles(saved_fields[step_index], edge_flips)).astype(jnp.bfloat16)
        pre_act = jnp.einsum('ih,nic->nhc', w_in32, patch_vals.astype(jnp.float32)) + b_in[None, :, None]
        hidden_vals = jax.nn.silu(pre_act).astype(jnp.bfloat16)
        scaled = STEP_SIZE * gradient
        level_grad = jnp.sum(scaled, axis=(0, 2)) / (TILES * COLS)
        tend_grad = (scaled - level_grad[None, :, None]).astype(jnp.bfloat16).astype(jnp.float32)
        grad_w_out = grad_w_out + jnp.einsum('nlc,nhc->lh', tend_grad, hidden_vals.astype(jnp.float32))
        hidden_grad = jnp.einsum('lh,nlc->nhc', w_out32, tend_grad)
        sigmoid_vals = jax.nn.sigmoid(pre_act)
        pre_grad = hidden_grad * sigmoid_vals * (1.0 + pre_act * (1.0 - sigmoid_vals))
        grad_b_in = grad_b_in + jnp.sum(pre_grad, axis=(0, 2))
        pre_low = pre_grad.astype(jnp.bfloat16).astype(jnp.float32)
        grad_w_in = grad_w_in + jnp.einsum('nic,nhc->ih', patch_vals.astype(jnp.float32), pre_low)
        patch_grad = jnp.einsum('ih,nhc->nic', w_in32, pre_low)
        gradient = gradient + unpad_tiles(scatter_patches(patch_grad), edge_flips).reshape(TILES, LEVELS, COLS)
    return (final_state, gradient, grad_w_in, grad_b_in, grad_w_out)
```

```python
import functools

import jax
import jax.numpy as jnp
from jax import lax
from jax.experimental import pallas as pl
from jax.experimental.pallas import tpu as pltpu
from jax.sharding import PartitionSpec as P

STEPS = 4
TILE_ROW = 4
STEP_SIZE = 0.25
LEAD = 8
MESH = pl.DeviceIdType.MESH
F32 = jnp.float32
BF16 = jnp.bfloat16

LANES = 128


def layout(width, rows):
    names = [("NW", 1), ("NE", 1), ("SW", 1), ("SE", 1), ("N", width), ("S", width), ("W", rows), ("E", rows)]
    place, at = {}, 0
    for name, size in names:
        place[name] = (at, size)
        at += -(-size // 8) * 8
    return place, at


def reduce_plan(tiles, subs, flat_rows):
    bits = [("sub", 1 << i) for i in range(subs.bit_length() - 1)]
    bits += [("tile", 1 << i) for i in range(tiles.bit_length() - 1)]
    unit = 16 * tiles * subs
    units = -(-flat_rows // unit)
    count = min(3, units)
    groups, at = [], 0
    for g in range(count):
        size = (units // count + (1 if g < units % count else 0)) * unit
        turning = bits[1:4]
        order = bits[:1] + turning[g:] + turning[:g] + bits[4:]
        groups.append((at, size, order))
        at += size
    return groups, at


def dot(a, b, dims, precision=None):
    return lax.dot_general(a, b, (dims, ((), ())), preferred_element_type=F32, precision=precision)


def tree_sum(parts):
    while len(parts) > 1:
        parts = [parts[i] + parts[i + 1] if i + 1 < len(parts) else parts[i] for i in range(0, len(parts), 2)]
    return parts[0]


def chain_kernel(
    tiles, subs, rows, width, levels, hidden,
    state_hbm, cot_hbm, w_in_hbm, b_in_hbm, w_out_hbm, flips_hbm,
    final_ref, grad_ref, whole,
    state_ref, cot_ref, w_in_ref, b_in_ref, w_out_ref, flips_ref, load_sem,
    gw_in_ref, gb_ref, gw_out_ref,
    flat, out_half, in_half, red_ssem, red_rsem, gat_ssem, gat_rsem,
    send, recv, sum_out, sum_in,
    padded, pad_grad, edge, field, gradient, totals, center, w_sum, hid, slope, patch,
    gp32, gp16, shifts,
    halo_ssem, halo_rsem, sum_ssem, sum_rsem,
):
    place, _ = layout(width, rows)
    cols = rows * width
    count = tiles * subs
    inv_total = 1.0 / (count * cols)
    me_t, me_s = lax.axis_index("tile"), lax.axis_index("sub")
    me = me_t * subs + me_s
    first, last = me_s == 0, me_s == subs - 1
    wide = width + 2 * LEAD
    in_width = w_in_ref.shape[0]
    unroll = count <= 64

    loads = [
        pltpu.make_async_copy(src, dst, load_sem.at[i])
        for i, (src, dst) in enumerate((
            (state_hbm, state_ref), (cot_hbm, cot_ref), (flips_hbm, flips_ref),
            (w_out_hbm, w_out_ref), (b_in_hbm, b_in_ref), (w_in_hbm, w_in_ref)))
    ]
    for load in loads:
        load.start()

    def device_at(by):
        other = lax.rem(me + by, count)
        return (other // subs, lax.rem(other, subs))

    barrier = pltpu.get_barrier_semaphore()

    def greet(by, carry):
        pl.semaphore_signal(barrier, inc=1, device_id=device_at(by), device_id_type=MESH)
        return carry

    lax.fori_loop(1, count, greet, 0, unroll=unroll)

    def tile_at(by):
        return lax.rem(me_t + by + 2 * tiles, tiles)

    def north_of(by):
        return (jnp.where(first, tile_at(by - TILE_ROW), tile_at(by)), jnp.where(first, subs - 1, me_s - 1))

    def south_of(by):
        return (jnp.where(last, tile_at(by + TILE_ROW), tile_at(by)), jnp.where(last, 0, me_s + 1))

    targets = {
        "N": north_of(0), "S": south_of(0), "W": (tile_at(-1), me_s), "E": (tile_at(1), me_s),
        "NW": north_of(-1), "NE": north_of(1), "SW": south_of(-1), "SE": south_of(1),
    }

    def halo_copies(p):
        out = []
        for i, (name, (at, size)) in enumerate(place.items()):
            out.append(pltpu.make_async_remote_copy(
                src_ref=send.at[p, pl.ds(at, size)], dst_ref=recv.at[p, pl.ds(at, size)],
                send_sem=halo_ssem.at[p, i], recv_sem=halo_rsem.at[p, i],
                device_id=targets[name], device_id_type=MESH))
        return out

    def start_halos(p):
        for copy in halo_copies(p):
            copy.start()

    def wait_halos(p):
        for copy in halo_copies(p):
            copy.wait()

    def start_sums(p, a, b):
        sum_out[p, 0:1] = jnp.concatenate([a, b], axis=1)

        def begin(by, carry):
            pltpu.make_async_remote_copy(
                src_ref=sum_out.at[p, pl.ds(0, 1)], dst_ref=sum_in.at[p, by - 1, pl.ds(0, 1)],
                send_sem=sum_ssem.at[p], recv_sem=sum_rsem.at[p],
                device_id=device_at(by), device_id_type=MESH).start()
            return carry

        lax.fori_loop(1, count, begin, 0, unroll=unroll)

    def wait_sums(p):
        pltpu.make_async_remote_copy(
            src_ref=sum_in.at[p, :, pl.ds(0, 1)], dst_ref=sum_in.at[p, :, pl.ds(0, 1)],
            send_sem=sum_ssem.at[p], recv_sem=sum_rsem.at[p],
            device_id=device_at(1), device_id_type=MESH).wait()
        if count <= 64:
            total = tree_sum([sum_out[p, 0:1]] + [sum_in[p, d, 0:1] for d in range(count - 1)])
        else:
            total = sum_out[p, 0:1] + jnp.sum(sum_in[p, :, 0:1], axis=0)
        return total[:, :levels], total[:, levels:]

    at_row = lax.broadcasted_iota(jnp.int32, (wide, wide), 0)
    at_col = lax.broadcasted_iota(jnp.int32, (wide, wide), 1)
    same = (at_row == at_col).astype(F32)
    turned = (at_row + at_col == wide - 1).astype(F32)
    diagonal = (
        lax.broadcasted_iota(jnp.int32, (levels, levels), 0) == lax.broadcasted_iota(jnp.int32, (levels, levels), 1)
    ).astype(F32)

    def column(line):
        return jnp.sum(diagonal * line, axis=1, keepdims=True)

    def seam_matrix(flag, here):
        mix = jnp.where(here, flag, 0).astype(F32)
        return turned * mix + same * (1.0 - mix)

    def send_field(p):
        for name, row in (("N", 0), ("S", rows - 1)):
            at = place[name][0]
            line = field[row * width:(row + 1) * width]
            send[p, at:at + width] = line
            for side, cell in (("W", 0), ("E", width - 1)):
                corner = place[name + side][0]
                send[p, corner:corner + 1] = line[cell:cell + 1]
        for name, cell in (("W", 0), ("E", width - 1)):
            at = place[name][0]
            for r in range(rows):
                send[p, at + r:at + r + 1] = field[r * width + cell:r * width + cell + 1]

    def pad_field(p, shift):
        for name, cell in (("E", LEAD - 1), ("W", LEAD + width)):
            at = place[name][0]
            for r in range(rows):
                padded[r + 1, cell:cell + 1] = recv[p, at + r:at + r + 1] - shift
        for name, row, flag in (("S", 0, 0), ("N", rows + 1, 1)):
            at = place[name][0]
            edge[LEAD:LEAD + width] = recv[p, at:at + width] - shift
            for side, cell in (("E", LEAD - 1), ("W", LEAD + width)):
                corner = place[name + side][0]
                edge[cell:cell + 1] = recv[p, corner:corner + 1] - shift
            padded[row] = dot(turns[flag].astype(BF16), edge[...].astype(BF16), ((1,), (0,)))

    edge[...] = jnp.zeros_like(edge)
    padded[...] = jnp.zeros_like(padded)
    center[...] = jnp.zeros_like(center)
    totals[...] = jnp.zeros_like(totals)
    nothing = jnp.zeros((1, levels), F32)
    loads[0].wait()
    field[...] = state_ref[0].T
    send_field(0)
    loads[1].wait()
    gradient[...] = cot_ref[0].T
    cot_sum = jnp.sum(gradient[...], axis=0, keepdims=True)
    pl.semaphore_wait(barrier, count - 1)
    start_halos(0)
    start_sums(0, nothing, cot_sum)
    loads[2].wait()
    turns = [
        seam_matrix(flips_ref[0:1, 0:1], first),
        seam_matrix(flips_ref[0:1, 1:2], last),
    ]
    gw_in_ref[...] = jnp.zeros_like(gw_in_ref)
    gb_ref[...] = jnp.zeros_like(gb_ref)
    gw_out_ref[...] = jnp.zeros_like(gw_out_ref)
    for load in loads[3:]:
        load.wait()
    w_sum[...] = w_in_ref[0:levels].astype(F32)
    for o in range(1, 9):
        w_sum[...] += w_in_ref[o * levels:(o + 1) * levels].astype(F32)

    def forward(k, carry):
        mid = center[0:1]
        padded[1:rows + 1, LEAD:LEAD + width, :] = (field[...] - mid).reshape(rows, width, levels)
        wait_halos(k)
        pad_field(k, mid)
        for a in range(3):
            for b in range(3):
                o = 3 * a + b
                piece = padded[a:a + rows, LEAD - 1 + b:LEAD - 1 + b + width, :]
                patch[k, :, o * levels:(o + 1) * levels] = piece.reshape(cols, levels).astype(BF16)
        act = dot(patch[k], w_in_ref[...], ((1,), (0,)))
        sum_a, sum_b = wait_sums(k)
        shift = sum_a * (STEP_SIZE * inv_total)
        totals[1:2] += sum_b
        move = mid - shift
        shifts[k, 0:1] = move
        act = act + (b_in_ref[...] + jnp.sum(w_sum[...] * column(move), axis=0, keepdims=True))
        sig = jax.nn.sigmoid(act)
        low = (act * sig).astype(BF16)
        hid[k] = low
        tendency = dot(low, w_out_ref[...], ((1,), (1,)))
        field[...] = (field[...] - shift) + STEP_SIZE * tendency
        own = jnp.sum(tendency, axis=0, keepdims=True)

        @pl.when(k < STEPS - 1)
        def _():
            send_field(k + 1)
            start_halos(k + 1)
            start_sums(k + 1, own, nothing)

        center[0:1] = own * (STEP_SIZE / cols)
        center[1:2] = own
        slope[k] = sig * (1.0 + act * (1.0 - sig))
        return carry

    lax.fori_loop(0, STEPS, forward, 0)

    def gradient_through(k, j):
        mid = jnp.sum(gradient[...], axis=0, keepdims=True) * (STEP_SIZE / cols)
        gh = dot((STEP_SIZE * gradient[...] - mid).astype(BF16), w_out_ref[...], ((1,), (0,)))

        @pl.when(j > 0)
        def _():
            sum_a, sum_b = wait_sums(STEPS + j - 1)
            totals[0:1] += sum_a
            totals[1:2] += sum_b

        level_grad = totals[1:2] * (STEP_SIZE * inv_total)
        lift = jnp.sum(w_out_ref[...].astype(F32) * column(mid - level_grad), axis=0, keepdims=True)
        gp = (gh + lift) * slope[k]
        gp32[...] = gp
        gp16[...] = gp.astype(BF16)
        return level_grad

    def spread(p, sums):
        gi = dot(gp16[...], w_in_ref[...], ((1,), (1,)))
        pad_grad[...] = jnp.zeros_like(pad_grad)
        if sums is not None:
            gi_sum = jnp.sum(gi, axis=0, keepdims=True)
            part = tree_sum([gi_sum[:, o * levels:(o + 1) * levels] for o in range(9)])
            start_sums(p, sums, part)
        for a in range(3):
            for b in range(3):
                o = 3 * a + b
                piece = gi[:, o * levels:(o + 1) * levels].reshape(rows, width, levels)
                pad_grad[a:a + rows, LEAD - 1 + b:LEAD - 1 + b + width, :] += piece
        for name, row, flag in (("N", 0, 0), ("S", rows + 1, 1)):
            at = place[name][0]
            edge[...] = dot(turns[flag], pad_grad[row], ((1,), (0,)), lax.Precision.HIGHEST)
            send[p, at:at + width] = edge[LEAD:LEAD + width]
            for side, cell in (("W", LEAD - 1), ("E", LEAD + width)):
                corner = place[name + side][0]
                send[p, corner:corner + 1] = edge[cell:cell + 1]
        for name, cell in (("W", LEAD - 1), ("E", LEAD + width)):
            at = place[name][0]
            for r in range(rows):
                send[p, at + r:at + r + 1] = pad_grad[r + 1, cell:cell + 1]
        start_halos(p)

    def weigh(k, level_grad):
        gp_sum = jnp.sum(gp32[...], axis=0, keepdims=True)
        gb_ref[...] += gp_sum
        back = column(shifts[k, 0:1]) * gp_sum
        gw = dot(patch[k], gp16[...], ((0,), (0,)))
        for o in range(9):
            part = slice(o * levels, (o + 1) * levels)
            gw_in_ref[part] += gw[part] + back
        low_gt = (STEP_SIZE * gradient[...] - level_grad).astype(BF16)
        gw_out_ref[...] += dot(low_gt, hid[k], ((0,), (0,)))

    def collect(p):
        for name, row in (("N", rows - 1), ("S", 0)):
            at = place[name][0]
            gradient[row * width:(row + 1) * width] += recv[p, at:at + width]
            for side, cell in (("W", width - 1), ("E", 0)):
                corner = place[name + side][0]
                gradient[row * width + cell:row * width + cell + 1] += recv[p, corner:corner + 1]
        for name, cell in (("W", width - 1), ("E", 0)):
            at = place[name][0]
            for r in range(rows):
                gradient[r * width + cell:r * width + cell + 1] += recv[p, at + r:at + r + 1]

    def backward(j, carry):
        k = STEPS - 1 - j
        p = STEPS + j
        level_grad = gradient_through(k, j)
        spread(p, jnp.where(j == 0, center[1:2], 0.0))
        weigh(k, level_grad)
        gradient[...] += pad_grad[1:rows + 1, LEAD:LEAD + width, :].reshape(cols, levels)
        wait_halos(p)
        collect(p)
        return carry

    lax.fori_loop(0, STEPS - 1, backward, 0)
    level_grad = gradient_through(0, STEPS - 1)
    weigh(0, level_grad)

    stride = in_width + levels + 8
    groups, flat_rows = reduce_plan(tiles, subs, stride * (hidden // LANES))
    for c in range(hidden // LANES):
        at, lanes = c * stride, slice(c * LANES, (c + 1) * LANES)
        flat[at:at + in_width] = gw_in_ref[:, lanes]
        flat[at + in_width:at + in_width + levels] = gw_out_ref[:, lanes]
        flat[at + in_width + levels:at + stride] = jnp.broadcast_to(gb_ref[:, lanes], (8, LANES))
    used = stride * (hidden // LANES)
    if flat_rows > used:
        flat[used:flat_rows] = jnp.zeros((flat_rows - used, LANES), F32)

    def bit_of(axis, step):
        index = me_t if axis == "tile" else me_s
        return lax.rem(index // step, 2)

    def peer_of(axis, step):
        if axis == "tile":
            return (me_t + step * (1 - 2 * bit_of(axis, step)), me_s)
        return (me_t, me_s + step * (1 - 2 * bit_of(axis, step)))

    def bases(group):
        start, size, order = group
        out, base = [], start
        for axis, step in order:
            out.append((base, size // 2))
            size = size // 2
            base = base + bit_of(axis, step) * size
        return out, base, size

    depth = len(groups[0][2])

    def reduce_copy(g, i):
        start, size, order = groups[g]
        half = size >> (i + 1)
        at = start + size - (size >> i)
        return pltpu.make_async_remote_copy(
            src_ref=out_half.at[pl.ds(at, half)], dst_ref=in_half.at[pl.ds(at, half)],
            send_sem=red_ssem.at[g, i], recv_sem=red_rsem.at[g, i],
            device_id=peer_of(*order[i]), device_id_type=MESH)

    def gather_copy(g, i):
        start, size, order = groups[g]
        part = size >> (i + 1)
        base = bases(groups[g])[0][i][0] + bit_of(*order[i]) * part
        rows_here = pl.ds(pl.multiple_of(base, 16), part)
        return pltpu.make_async_remote_copy(
            src_ref=whole.at[rows_here], dst_ref=whole.at[rows_here],
            send_sem=gat_ssem.at[g, i], recv_sem=gat_rsem.at[g, i],
            device_id=peer_of(*order[i]), device_id_type=MESH)

    for i in range(depth + 1):
        for g, (start, size, order) in enumerate(groups):
            levels_of = bases((start, size, order))
            if i > 0:
                reduce_copy(g, i - 1).wait()
                base, half = levels_of[0][i - 1]
                at = start + size - (size >> (i - 1))
                kept = pl.ds(pl.multiple_of(base + bit_of(*order[i - 1]) * half, 16), half)
                flat[kept] = flat[kept] + in_half[at:at + half].astype(F32)
            if i < depth:
                base, half = levels_of[0][i]
                at = start + size - (size >> i)
                away = pl.ds(pl.multiple_of(base + (1 - bit_of(*order[i])) * half, 16), half)
                out_half[at:at + half] = flat[away].astype(BF16)
                reduce_copy(g, i).start()
            else:
                own = pl.ds(pl.multiple_of(levels_of[1], 16), levels_of[2])
                whole[own] = flat[own].astype(BF16)
                gather_copy(g, depth - 1).start()
        if i == 1:
            spread(2 * STEPS - 1, None)
            gradient[...] += pad_grad[1:rows + 1, LEAD:LEAD + width, :].reshape(cols, levels)
            final_ref[0] = (field[...] - totals[0:1] * (STEP_SIZE * inv_total)).T
        if i == depth - 1:
            wait_halos(2 * STEPS - 1)
            collect(2 * STEPS - 1)
            grad_ref[0] = gradient[...].T
    for i in reversed(range(depth)):
        for g in range(len(groups)):
            gather_copy(g, i).wait()
            if i > 0:
                gather_copy(g, i - 1).start()


def finish_kernel(hidden, final_in, grad_in, whole, final_ref, grad_ref, gw_in_ref, gb_ref, gw_out_ref, wide_in, wide_b, wide_out, sem):
    in_width, levels = gw_in_ref.shape[0], gw_out_ref.shape[0]
    stride = in_width + levels + 8
    copies = [
        pltpu.make_async_copy(final_in, final_ref, sem.at[0]),
        pltpu.make_async_copy(grad_in, grad_ref, sem.at[1]),
    ]
    for copy in copies:
        copy.start()
    chunks = hidden // LANES
    for c in range(chunks):
        at, lanes = c * stride, slice(c * LANES, (c + 1) * LANES)
        wide_in[c] = whole[at:at + in_width].astype(F32)
        copies.append(pltpu.make_async_copy(wide_in.at[c], gw_in_ref.at[:, pl.ds(c * LANES, LANES)], sem.at[4 + c]))
        copies[-1].start()
        wide_out[:, lanes] = whole[at + in_width:at + in_width + levels].astype(F32)
        tail = whole[at + in_width + levels - 8:at + stride].astype(F32)
        wide_b[:, lanes] = tail[8:9]
    copies.append(pltpu.make_async_copy(wide_out, gw_out_ref, sem.at[2]))
    copies[-1].start()
    copies.append(pltpu.make_async_copy(wide_b, gb_ref, sem.at[3]))
    copies[-1].start()
    for copy in copies:
        copy.wait()


def shards(tiles, subs, initial_state, cotangent, w_in, b_in, w_out, edge_flips):
    _, levels, cols = initial_state.shape
    in_width, hidden = w_in.shape
    side = 1
    while side * side < cols * subs:
        side += 1
    rows, width = side // subs, side
    _, buffer_rows = layout(width, rows)
    phases = 2 * STEPS
    count = tiles * subs
    groups, flat_rows = reduce_plan(tiles, subs, (in_width + levels + 8) * (hidden // LANES))
    depth = len(groups[0][2])
    wide = width + 2 * LEAD
    vmem = pl.BlockSpec(memory_space=pltpu.VMEM)
    hbm = pl.BlockSpec(memory_space=pltpu.HBM)
    final, grad, whole = pl.pallas_call(
        functools.partial(chain_kernel, tiles, subs, rows, width, levels, hidden),
        out_shape=(
            jax.ShapeDtypeStruct(initial_state.shape, F32),
            jax.ShapeDtypeStruct(initial_state.shape, F32),
            jax.ShapeDtypeStruct((flat_rows, LANES), BF16),
        ),
        in_specs=[hbm] * 6,
        out_specs=[vmem] * 3,
        scratch_shapes=[
            pltpu.VMEM(initial_state.shape, F32),
            pltpu.VMEM(initial_state.shape, F32),
            pltpu.VMEM((in_width, hidden), BF16),
            pltpu.VMEM((1, hidden), F32),
            pltpu.VMEM((levels, hidden), BF16),
            pltpu.VMEM(edge_flips.shape, jnp.int32),
            pltpu.SemaphoreType.DMA((6,)),
            pltpu.VMEM((in_width, hidden), F32),
            pltpu.VMEM((1, hidden), F32),
            pltpu.VMEM((levels, hidden), F32),
            pltpu.VMEM((flat_rows, LANES), F32),
            pltpu.VMEM((flat_rows, LANES), BF16),
            pltpu.VMEM((flat_rows, LANES), BF16),
            pltpu.SemaphoreType.DMA((len(groups), depth)),
            pltpu.SemaphoreType.DMA((len(groups), depth)),
            pltpu.SemaphoreType.DMA((len(groups), depth)),
            pltpu.SemaphoreType.DMA((len(groups), depth)),
            pltpu.VMEM((phases, buffer_rows, levels), F32),
            pltpu.VMEM((phases, buffer_rows, levels), F32),
            pltpu.VMEM((phases, 8, 2 * levels), F32),
            pltpu.VMEM((phases, count - 1, 8, 2 * levels), F32),
            pltpu.VMEM((rows + 2, wide, levels), F32),
            pltpu.VMEM((rows + 2, wide, levels), F32),
            pltpu.VMEM((wide, levels), F32),
            pltpu.VMEM((cols, levels), F32),
            pltpu.VMEM((cols, levels), F32),
            pltpu.VMEM((8, levels), F32),
            pltpu.VMEM((8, levels), F32),
            pltpu.VMEM((levels, hidden), F32),
            pltpu.VMEM((STEPS, cols, hidden), BF16),
            pltpu.VMEM((STEPS, cols, hidden), F32),
            pltpu.VMEM((STEPS, cols, in_width), BF16),
            pltpu.VMEM((cols, hidden), F32),
            pltpu.VMEM((cols, hidden), BF16),
            pltpu.VMEM((STEPS, 8, levels), F32),
            pltpu.SemaphoreType.DMA((phases, 8)),
            pltpu.SemaphoreType.DMA((phases, 8)),
            pltpu.SemaphoreType.DMA((phases,)),
            pltpu.SemaphoreType.DMA((phases,)),
        ],
        compiler_params=pltpu.CompilerParams(has_side_effects=True, collective_id=0, vmem_limit_bytes=44 * 1024 * 1024),
        name="chain",
    )(*[pltpu.with_memory_space_constraint(v, pltpu.HBM) for v in (initial_state, cotangent, w_in, b_in[None, :], w_out, edge_flips)])
    final, grad, gw_in, gb, gw_out = pl.pallas_call(
        functools.partial(finish_kernel, hidden),
        out_shape=(
            jax.ShapeDtypeStruct(initial_state.shape, F32),
            jax.ShapeDtypeStruct(initial_state.shape, F32),
            jax.ShapeDtypeStruct((in_width, hidden), F32),
            jax.ShapeDtypeStruct((1, hidden), F32),
            jax.ShapeDtypeStruct((levels, hidden), F32),
        ),
        in_specs=[vmem] * 3,
        out_specs=[hbm] * 5,
        scratch_shapes=[
            pltpu.VMEM((hidden // LANES, in_width, LANES), F32),
            pltpu.VMEM((1, hidden), F32),
            pltpu.VMEM((levels, hidden), F32),
            pltpu.SemaphoreType.DMA((4 + hidden // LANES,)),
        ],
        compiler_params=pltpu.CompilerParams(vmem_limit_bytes=8 * 1024 * 1024),
        name="finish",
    )(final, grad, whole)
    return (final, grad, gw_in, gb[0], gw_out)


def solution(mesh):
    in_specs = (P("tile", None, "sub"), P("tile", None, "sub"), P(), P(), P(), P("tile", None))
    out_specs = (P("tile", None, "sub"), P("tile", None, "sub"), P(), P(), P())
    body = functools.partial(shards, mesh.shape["tile"], mesh.shape["sub"])
    return jax.shard_map(body, mesh=mesh, in_specs=in_specs, out_specs=out_specs, check_vma=False)
```

```python
import functools

import jax
import jax.numpy as jnp
from jax import lax
from jax.experimental import pallas as pl
from jax.experimental.pallas import tpu as pltpu
from jax.sharding import PartitionSpec as P

STEPS = 4
TILE_ROW = 4
STEP_SIZE = 0.25
LEAD = 8
MESH = pl.DeviceIdType.MESH
F32 = jnp.float32
BF16 = jnp.bfloat16

LANES = 128


def layout(width, rows):
    names = [("NW", 1), ("NE", 1), ("SW", 1), ("SE", 1), ("N", width), ("S", width), ("W", rows), ("E", rows)]
    place, at = {}, 0
    for name, size in names:
        place[name] = (at, size)
        at += -(-size // 8) * 8
    return place, at


def reduce_plan(tiles, subs, flat_rows):
    sub_bits = [("sub", 1 << i) for i in range(subs.bit_length() - 1)]
    tile_bits = [("tile", 1 << i) for i in range(tiles.bit_length() - 1)]
    rest = sub_bits[1:] + tile_bits
    pairs = [tuple(rest[i:i + 2]) for i in range(0, len(rest), 2)]
    orders = [[tuple(sub_bits[:1])] + pairs, [tuple(sub_bits[:1])] + pairs[1:2] + pairs[:1] + pairs[2:]]
    unit = 8 * tiles * subs
    units = -(-flat_rows // unit)
    shares = [0, 0, 0, 0]
    for n, part in enumerate((0.3, 0.5, 0.8, 1.0)):
        shares[n] = int(round(units * part)) - sum(shares[:n])
    groups, at = [], 0
    for n, share in enumerate(shares):
        if share:
            groups.append((at, share * unit, orders[n % 2]))
            at += share * unit
    return groups, at


def dot(a, b, dims, precision=None):
    return lax.dot_general(a, b, (dims, ((), ())), preferred_element_type=F32, precision=precision)


def tree_sum(parts):
    while len(parts) > 1:
        parts = [parts[i] + parts[i + 1] if i + 1 < len(parts) else parts[i] for i in range(0, len(parts), 2)]
    return parts[0]


def chain_kernel(
    tiles, subs, rows, width, levels, hidden,
    state_hbm, cot_hbm, w_in_hbm, b_in_hbm, w_out_hbm, flips_hbm,
    final_ref, grad_ref, whole, gb_ref,
    state_ref, cot_ref, w_in_ref, b_in_ref, w_out_ref, flips_ref, load_sem,
    flat, out_half, in_half, red_ssem, red_rsem, gat_ssem, gat_rsem,
    gb_sum, gb_out, gb_in, gb_far, gb_ssem, gb_rsem,
    send, recv, sum_out, sum_in,
    padded, pad_grad, edge, lines, ends, field, gradient, totals, center, w_sum, hid, slope, patch, patch_t,
    rim, pre, gp_sum, gp16, shifts,
    halo_ssem, halo_rsem, sum_ssem, sum_rsem,
):
    place, _ = layout(width, rows)
    cols = rows * width
    count = tiles * subs
    inv_total = 1.0 / (count * cols)
    me_t, me_s = lax.axis_index("tile"), lax.axis_index("sub")
    me = me_t * subs + me_s
    first, last = me_s == 0, me_s == subs - 1
    wide = width + 2 * LEAD
    in_width = w_in_ref.shape[0]
    stride = in_width + levels
    chunks = hidden // LANES
    groups, flat_rows = reduce_plan(tiles, subs, stride * chunks)
    rim_rows = -(-rows // 16) * 16
    unroll = count <= 64

    loads = [
        pltpu.make_async_copy(src, dst, load_sem.at[i])
        for i, (src, dst) in enumerate((
            (state_hbm, state_ref), (cot_hbm, cot_ref), (flips_hbm, flips_ref),
            (w_out_hbm, w_out_ref), (b_in_hbm, b_in_ref), (w_in_hbm, w_in_ref)))
    ]
    for load in loads:
        load.start()

    def device_at(by):
        other = lax.rem(me + by, count)
        return (other // subs, lax.rem(other, subs))

    barrier = pltpu.get_barrier_semaphore()

    def greet(by, carry):
        pl.semaphore_signal(barrier, inc=1, device_id=device_at(by), device_id_type=MESH)
        return carry

    lax.fori_loop(1, count, greet, 0, unroll=unroll)

    def tile_at(by):
        return lax.rem(me_t + by + 2 * tiles, tiles)

    def north_of(by):
        return (jnp.where(first, tile_at(by - TILE_ROW), tile_at(by)), jnp.where(first, subs - 1, me_s - 1))

    def south_of(by):
        return (jnp.where(last, tile_at(by + TILE_ROW), tile_at(by)), jnp.where(last, 0, me_s + 1))

    targets = {
        "N": north_of(0), "S": south_of(0), "W": (tile_at(-1), me_s), "E": (tile_at(1), me_s),
        "NW": north_of(-1), "NE": north_of(1), "SW": south_of(-1), "SE": south_of(1),
    }

    def halo_copies(p):
        out = []
        for i, (name, (at, size)) in enumerate(place.items()):
            out.append(pltpu.make_async_remote_copy(
                src_ref=send.at[p, pl.ds(at, size)], dst_ref=recv.at[p, pl.ds(at, size)],
                send_sem=halo_ssem.at[p, i], recv_sem=halo_rsem.at[p, i],
                device_id=targets[name], device_id_type=MESH))
        return out

    def start_halos(p):
        for copy in halo_copies(p):
            copy.start()

    def wait_halos(p):
        for copy in halo_copies(p):
            copy.wait()

    def start_sums(p, a, b):
        sum_out[p, 0:1] = jnp.concatenate([a, b], axis=1)

        def begin(by, carry):
            pltpu.make_async_remote_copy(
                src_ref=sum_out.at[p, pl.ds(0, 1)], dst_ref=sum_in.at[p, by - 1, pl.ds(0, 1)],
                send_sem=sum_ssem.at[p], recv_sem=sum_rsem.at[p],
                device_id=device_at(by), device_id_type=MESH).start()
            return carry

        lax.fori_loop(1, count, begin, 0, unroll=unroll)

    def wait_sums(p):
        pltpu.make_async_remote_copy(
            src_ref=sum_in.at[p, :, pl.ds(0, 1)], dst_ref=sum_in.at[p, :, pl.ds(0, 1)],
            send_sem=sum_ssem.at[p], recv_sem=sum_rsem.at[p],
            device_id=device_at(1), device_id_type=MESH).wait()
        if count <= 64:
            total = tree_sum([sum_out[p, 0:1]] + [sum_in[p, d, 0:1] for d in range(count - 1)])
        else:
            total = sum_out[p, 0:1] + jnp.sum(sum_in[p, :, 0:1], axis=0)
        return total[:, :levels], total[:, levels:]

    at_row = lax.broadcasted_iota(jnp.int32, (wide, wide), 0)
    at_col = lax.broadcasted_iota(jnp.int32, (wide, wide), 1)
    same = (at_row == at_col).astype(F32)
    turned = (at_row + at_col == wide - 1).astype(F32)
    diagonal = (
        lax.broadcasted_iota(jnp.int32, (levels, levels), 0) == lax.broadcasted_iota(jnp.int32, (levels, levels), 1)
    ).astype(F32)

    def column(flat_line):
        return jnp.sum(diagonal * flat_line, axis=1, keepdims=True)

    def turn_exact(turn, value):
        high = value.astype(BF16)
        left = value - high.astype(F32)
        middle = left.astype(BF16)
        low = (left - middle.astype(F32)).astype(BF16)
        parts = dot(turn.astype(BF16), jnp.concatenate([high, middle, low], axis=1), ((1,), (0,)))
        return parts[:, :levels] + parts[:, levels:2 * levels] + parts[:, 2 * levels:]

    def seam_matrix(flag, here):
        mix = jnp.where(here, flag, 0).astype(F32)
        return turned * mix + same * (1.0 - mix)

    def send_field(p):
        for name, row in (("N", 0), ("S", rows - 1)):
            at = place[name][0]
            line = field[row * width:(row + 1) * width]
            send[p, at:at + width] = line
            for side, cell in (("W", 0), ("E", width - 1)):
                corner = place[name + side][0]
                send[p, corner:corner + 1] = line[cell:cell + 1]
        for name, cell in (("W", 0), ("E", width - 1)):
            at = place[name][0]
            for r in range(rows):
                send[p, at + r:at + r + 1] = field[r * width + cell:r * width + cell + 1]

    def gather_patch():
        for a in range(3):
            for b in range(3):
                o = 3 * a + b
                piece = padded[a:a + rows, LEAD - 1 + b:LEAD - 1 + b + width, :]
                patch[:, o * levels:(o + 1) * levels] = piece.reshape(cols, levels).astype(BF16)

    def gather_rim(p, shift):
        for n, name in enumerate(("S", "N")):
            at = place[name][0]
            edge[LEAD:LEAD + width] = recv[p, at:at + width] - shift
            for side, cell in (("E", LEAD - 1), ("W", LEAD + width)):
                corner = place[name + side][0]
                edge[cell:cell + 1] = recv[p, corner:corner + 1] - shift
            lines[n] = dot(turns[n].astype(BF16), edge[...].astype(BF16), ((1,), (0,)))
            for b in range(3):
                o = 6 * n + b
                rim[n * width:(n + 1) * width, o * levels:(o + 1) * levels] = (
                    lines[n, LEAD - 1 + b:LEAD - 1 + b + width].astype(BF16))
        for n, name in enumerate(("E", "W")):
            at = place[name][0]
            ends[n, LEAD:LEAD + rows] = recv[p, at:at + rows] - shift
            at = 2 * width + n * rim_rows
            for a in range(3):
                o = 3 * a + 2 * n
                rim[at:at + rows, o * levels:(o + 1) * levels] = (
                    ends[n, LEAD - 1 + a:LEAD - 1 + a + rows].astype(BF16))

    def add_rim():
        extra = dot(rim[...], w_in_ref[...], ((1,), (0,)))
        pre[0:width] += extra[0:width]
        pre[cols - width:cols] += extra[width:2 * width]
        for n, cell in ((0, 0), (1, width - 1)):
            for r in range(rows):
                at, row = r * width + cell, 2 * width + n * rim_rows + r
                pre[at:at + 1] += extra[row:row + 1]

    def whole_patch(k):
        for n, row in ((0, 0), (1, rows + 1)):
            padded[row] = lines[n]
        for n, cell in ((0, LEAD - 1), (1, LEAD + width)):
            for r in range(rows):
                padded[r + 1, cell:cell + 1] = ends[n, LEAD + r:LEAD + r + 1]
        gather_patch()
        patch_t[k] = patch[...].T
        for row in (0, rows + 1):
            padded[row] = jnp.zeros((wide, levels), F32)
        for cell in (LEAD - 1, LEAD + width):
            padded[1:rows + 1, cell:cell + 1] = jnp.zeros((rows, 1, levels), F32)

    edge[...] = jnp.zeros_like(edge)
    padded[...] = jnp.zeros_like(padded)
    center[...] = jnp.zeros_like(center)
    totals[...] = jnp.zeros_like(totals)
    nothing = jnp.zeros((1, levels), F32)
    loads[0].wait()
    field[...] = state_ref[0].T
    send_field(0)
    loads[1].wait()
    gradient[...] = cot_ref[0].T
    cot_sum = jnp.sum(gradient[...], axis=0, keepdims=True)
    pl.semaphore_wait(barrier, count - 1)
    start_halos(0)
    start_sums(0, nothing, cot_sum)
    loads[2].wait()
    turns = [
        seam_matrix(flips_ref[0:1, 0:1], first),
        seam_matrix(flips_ref[0:1, 1:2], last),
    ]
    flat[...] = jnp.zeros_like(flat)
    gb_sum[...] = jnp.zeros_like(gb_sum)
    ends[...] = jnp.zeros_like(ends)
    rim[...] = jnp.zeros_like(rim)
    for load in loads[3:]:
        load.wait()
    w_sum[...] = w_in_ref[0:levels].astype(F32)
    for o in range(1, 9):
        w_sum[...] += w_in_ref[o * levels:(o + 1) * levels].astype(F32)

    def forward(k, carry):
        mid = center[0:1]
        padded[1:rows + 1, LEAD:LEAD + width, :] = (field[...] - mid).reshape(rows, width, levels)
        gather_patch()
        pre[...] = dot(patch[...], w_in_ref[...], ((1,), (0,)))
        wait_halos(k)
        gather_rim(k, mid)
        add_rim()
        sum_a, sum_b = wait_sums(k)
        shift = sum_a * (STEP_SIZE * inv_total)
        totals[1:2] += sum_b
        move = mid - shift
        shifts[k, 0:1] = move
        act = pre[...] + (b_in_ref[...] + jnp.sum(w_sum[...] * column(move), axis=0, keepdims=True))
        sig = jax.nn.sigmoid(act)
        low = (act * sig).astype(BF16)
        hid[k] = low
        tendency = dot(low, w_out_ref[...], ((1,), (1,)))
        field[...] = (field[...] - shift) + STEP_SIZE * tendency
        own = jnp.sum(tendency, axis=0, keepdims=True)

        @pl.when(k < STEPS - 1)
        def _():
            send_field(k + 1)
            start_halos(k + 1)
            start_sums(k + 1, own, nothing)

        center[0:1] = own * (STEP_SIZE / cols)
        center[1:2] = own
        slope[k] = sig * (1.0 + act * (1.0 - sig))
        whole_patch(k)
        return carry

    lax.fori_loop(0, STEPS, forward, 0)

    def gradient_through(k, j):
        mid = jnp.sum(gradient[...], axis=0, keepdims=True) * (STEP_SIZE / cols)
        gh = dot((STEP_SIZE * gradient[...] - mid).astype(BF16), w_out_ref[...], ((1,), (0,)))

        @pl.when(j > 0)
        def _():
            sum_a, sum_b = wait_sums(STEPS + j - 1)
            totals[0:1] += sum_a
            totals[1:2] += sum_b

        level_grad = totals[1:2] * (STEP_SIZE * inv_total)
        lift = jnp.sum(w_out_ref[...].astype(F32) * column(mid - level_grad), axis=0, keepdims=True)
        gp = (gh + lift) * slope[k]
        gp16[...] = gp.astype(BF16)
        gp_sum[0:1] = jnp.sum(gp, axis=0, keepdims=True)
        return level_grad

    def spread(p, sums):
        gi = dot(gp16[...], w_in_ref[...], ((1,), (1,)))
        pad_grad[...] = jnp.zeros_like(pad_grad)
        if sums is not None:
            gi_sum = jnp.sum(gi, axis=0, keepdims=True)
            start_sums(p, sums, tree_sum([gi_sum[:, o * levels:(o + 1) * levels] for o in range(9)]))
        for a in range(3):
            for b in range(3):
                o = 3 * a + b
                piece = gi[:, o * levels:(o + 1) * levels].reshape(rows, width, levels)
                pad_grad[a:a + rows, LEAD - 1 + b:LEAD - 1 + b + width, :] += piece
        for n, (name, row) in enumerate((("N", 0), ("S", rows + 1))):
            at = place[name][0]
            edge[...] = turn_exact(turns[n], pad_grad[row])
            send[p, at:at + width] = edge[LEAD:LEAD + width]
            for side, cell in (("W", LEAD - 1), ("E", LEAD + width)):
                corner = place[name + side][0]
                send[p, corner:corner + 1] = edge[cell:cell + 1]
        for name, cell in (("W", LEAD - 1), ("E", LEAD + width)):
            at = place[name][0]
            for r in range(rows):
                send[p, at + r:at + r + 1] = pad_grad[r + 1, cell:cell + 1]
        start_halos(p)

    def keep():
        gradient[...] += pad_grad[1:rows + 1, LEAD:LEAD + width, :].reshape(cols, levels)

    def weigh(k, low_gt, c, many):
        lanes = slice(c * LANES, (c + many) * LANES)
        back = column(shifts[k, 0:1]) * gp_sum[0:1, lanes]
        gw = dot(patch_t[k], gp16[:, lanes], ((1,), (0,)))
        gw_out = dot(low_gt, hid[k, :, lanes], ((1,), (0,)))
        for n in range(many):
            at, part = (c + n) * stride, slice(n * LANES, (n + 1) * LANES)
            for o in range(9):
                flat[at + o * levels:at + (o + 1) * levels] += gw[o * levels:(o + 1) * levels, part] + back[:, part]
            flat[at + in_width:at + stride] += gw_out[:, part]

    def gradient_low(level_grad):
        return (STEP_SIZE * gradient[...] - level_grad).T.astype(BF16)

    def collect(p):
        for name, row in (("N", rows - 1), ("S", 0)):
            at = place[name][0]
            gradient[row * width:(row + 1) * width] += recv[p, at:at + width]
            for side, cell in (("W", width - 1), ("E", 0)):
                corner = place[name + side][0]
                gradient[row * width + cell:row * width + cell + 1] += recv[p, corner:corner + 1]
        for name, cell in (("W", width - 1), ("E", 0)):
            at = place[name][0]
            for r in range(rows):
                gradient[r * width + cell:r * width + cell + 1] += recv[p, at + r:at + r + 1]

    def backward(j, carry):
        k = STEPS - 1 - j
        p = STEPS + j
        level_grad = gradient_through(k, j)
        spread(p, jnp.where(j == 0, center[1:2], 0.0))
        low_gt = gradient_low(level_grad)
        keep()
        gb_sum[...] += gp_sum[0:1]
        weigh(k, low_gt, 0, chunks)
        wait_halos(p)
        collect(p)
        return carry

    lax.fori_loop(0, STEPS - 1, backward, 0)
    level_grad = gradient_through(0, STEPS - 1)
    low_gt = gradient_low(level_grad)

    def bit_of(bit):
        axis, step = bit
        return lax.rem((me_t if axis == "tile" else me_s) // step, 2)

    def peer_of(bits, mask):
        at = {"tile": me_t, "sub": me_s}
        for i, (axis, step) in enumerate(bits):
            if mask >> i & 1:
                at[axis] = at[axis] + step * (1 - 2 * bit_of((axis, step)))
        return (at["tile"], at["sub"])

    def place_of(bits, mask):
        index = 0
        for i, bit in enumerate(bits):
            index = index + (1 - bit_of(bit) if mask >> i & 1 else bit_of(bit)) * (1 << i)
        return index

    stages = []
    for start, size, order in groups:
        base, at, found = start, start, []
        for bits in order:
            piece = size >> len(bits)
            found.append((base, piece, at, bits))
            at += size - piece
            base = base + place_of(bits, 0) * piece
            size = piece
        stages.append((found, base, size))

    def rows_at(base, piece):
        return pl.ds(pl.multiple_of(base, 8), piece)

    def reduce_copies(g, i):
        base, piece, at, bits = stages[g][0][i]
        return [pltpu.make_async_remote_copy(
            src_ref=out_half.at[pl.ds(at + (m - 1) * piece, piece)],
            dst_ref=in_half.at[pl.ds(at + (m - 1) * piece, piece)],
            send_sem=red_ssem.at[g, i, m - 1], recv_sem=red_rsem.at[g, i, m - 1],
            device_id=peer_of(bits, m), device_id_type=MESH) for m in range(1, 1 << len(bits))]

    def reduce_start(g, i):
        base, piece, at, bits = stages[g][0][i]
        for m, copy in enumerate(reduce_copies(g, i), 1):
            away = flat[rows_at(base + place_of(bits, m) * piece, piece)]
            out_half[at + (m - 1) * piece:at + m * piece] = away.astype(BF16)
            copy.start()

    def reduce_wait(g, i):
        base, piece, at, bits = stages[g][0][i]
        own = rows_at(base + place_of(bits, 0) * piece, piece)
        total = flat[own]
        for m, copy in enumerate(reduce_copies(g, i), 1):
            copy.wait()
            total = total + in_half[at + (m - 1) * piece:at + m * piece].astype(F32)
        flat[own] = total

    def gather_copies(g, i):
        base, piece, at, bits = stages[g][0][i]
        own = rows_at(base + place_of(bits, 0) * piece, piece)
        return [pltpu.make_async_remote_copy(
            src_ref=whole.at[own], dst_ref=whole.at[own],
            send_sem=gat_ssem.at[g, i, m - 1], recv_sem=gat_rsem.at[g, i, m - 1],
            device_id=peer_of(bits, m), device_id_type=MESH) for m in range(1, 1 << len(bits))]

    near = tuple([("sub", 1 << i) for i in range(subs.bit_length() - 1)] + [("tile", 1)])
    far = tuple(("tile", 1 << i) for i in range(1, tiles.bit_length() - 1))

    def bias_copies(n):
        bits, source, slots = ((near, gb_out, gb_in), (far, gb_ref, gb_far))[n]
        return [pltpu.make_async_remote_copy(
            src_ref=source, dst_ref=slots.at[place_of(bits, 0)], send_sem=gb_ssem.at[n, m - 1], recv_sem=gb_rsem.at[n, m - 1],
            device_id=peer_of(bits, m), device_id_type=MESH) for m in range(1, 1 << len(bits))]

    def bias_start(n):
        bits, source, slots = ((near, gb_out, gb_in), (far, gb_ref, gb_far))[n]
        slots[place_of(bits, 0)] = source[...]
        for copy in bias_copies(n):
            copy.start()

    def bias_wait(n):
        for copy in bias_copies(n):
            copy.wait()
        slots = (gb_in, gb_far)[n]
        gb_ref[...] = tree_sum([slots[d] for d in range(slots.shape[0])])

    for c in range(chunks):
        lanes = slice(c * LANES, (c + 1) * LANES)
        gb_out[c:c + 1] = gb_sum[0:1, lanes] + gp_sum[0:1, lanes]
    bias_start(0)
    started = 0
    for c in range(0, chunks, 2):
        weigh(0, low_gt, c, 2)
        while started < len(groups) and (c + 2 == chunks or groups[started][0] + groups[started][1] <= (c + 2) * stride):
            reduce_start(started, 0)
            started += 1
    depth = max(len(order) for _, _, order in groups)
    for i in range(1, depth + 1):
        for g in range(len(groups)):
            reduce_wait(g, i - 1)
            if i < depth:
                reduce_start(g, i)
            else:
                _, base, size = stages[g]
                own = rows_at(base, size)
                whole[own] = flat[own].astype(BF16)
                for copy in gather_copies(g, depth - 1):
                    copy.start()
        if i == 1:
            spread(2 * STEPS - 1, None)
            keep()
            final_ref[0] = (field[...] - totals[0:1] * (STEP_SIZE * inv_total)).T
            bias_wait(0)
            bias_start(1)
        if i == 2:
            wait_halos(2 * STEPS - 1)
            collect(2 * STEPS - 1)
            grad_ref[0] = gradient[...].T
            bias_wait(1)
    for i in reversed(range(depth)):
        for g in range(len(groups)):
            for copy in gather_copies(g, i):
                copy.wait()
            if i > 0:
                for copy in gather_copies(g, i - 1):
                    copy.start()


def finish_kernel(hidden, final_in, grad_in, whole, gb_in, final_ref, grad_ref, gw_in_ref, gb_ref, gw_out_ref, wide_in, wide_out, sem):
    in_width, levels = gw_in_ref.shape[0], gw_out_ref.shape[0]
    stride = in_width + levels
    copies = [
        pltpu.make_async_copy(final_in, final_ref, sem.at[0]),
        pltpu.make_async_copy(grad_in, grad_ref, sem.at[1]),
        pltpu.make_async_copy(gb_in, gb_ref, sem.at[3]),
    ]
    for copy in copies:
        copy.start()
    for c in range(hidden // LANES):
        at, lanes = c * stride, slice(c * LANES, (c + 1) * LANES)
        wide_in[c] = whole[at:at + in_width].astype(F32)
        copies.append(pltpu.make_async_copy(wide_in.at[c], gw_in_ref.at[:, pl.ds(c * LANES, LANES)], sem.at[4 + c]))
        copies[-1].start()
        wide_out[:, lanes] = whole[at + in_width:at + stride].astype(F32)
    copies.append(pltpu.make_async_copy(wide_out, gw_out_ref, sem.at[2]))
    copies[-1].start()
    for copy in copies:
        copy.wait()


def shards(tiles, subs, initial_state, cotangent, w_in, b_in, w_out, edge_flips):
    _, levels, cols = initial_state.shape
    in_width, hidden = w_in.shape
    side = 1
    while side * side < cols * subs:
        side += 1
    rows, width = side // subs, side
    _, buffer_rows = layout(width, rows)
    phases = 2 * STEPS
    count = tiles * subs
    groups, flat_rows = reduce_plan(tiles, subs, (in_width + levels) * (hidden // LANES))
    depth = len(groups[0][2])
    chunks = hidden // LANES
    rim_rows = -(-rows // 16) * 16
    most = max(2 * subs, tiles // 2)
    wide = width + 2 * LEAD
    vmem = pl.BlockSpec(memory_space=pltpu.VMEM)
    hbm = pl.BlockSpec(memory_space=pltpu.HBM)
    final, grad, whole, gb = pl.pallas_call(
        functools.partial(chain_kernel, tiles, subs, rows, width, levels, hidden),
        out_shape=(
            jax.ShapeDtypeStruct(initial_state.shape, F32),
            jax.ShapeDtypeStruct(initial_state.shape, F32),
            jax.ShapeDtypeStruct((flat_rows, LANES), BF16),
            jax.ShapeDtypeStruct((chunks, LANES), F32),
        ),
        in_specs=[hbm] * 6,
        out_specs=[vmem] * 4,
        scratch_shapes=[
            pltpu.VMEM(initial_state.shape, F32),
            pltpu.VMEM(initial_state.shape, F32),
            pltpu.VMEM((in_width, hidden), BF16),
            pltpu.VMEM((1, hidden), F32),
            pltpu.VMEM((levels, hidden), BF16),
            pltpu.VMEM(edge_flips.shape, jnp.int32),
            pltpu.SemaphoreType.DMA((6,)),
            pltpu.VMEM((flat_rows, LANES), F32),
            pltpu.VMEM((flat_rows, LANES), BF16),
            pltpu.VMEM((flat_rows, LANES), BF16),
            pltpu.SemaphoreType.DMA((len(groups), depth, 3)),
            pltpu.SemaphoreType.DMA((len(groups), depth, 3)),
            pltpu.SemaphoreType.DMA((len(groups), depth, 3)),
            pltpu.SemaphoreType.DMA((len(groups), depth, 3)),
            pltpu.VMEM((1, hidden), F32),
            pltpu.VMEM((chunks, LANES), F32),
            pltpu.VMEM((2 * subs, chunks, LANES), F32),
            pltpu.VMEM((tiles // 2, chunks, LANES), F32),
            pltpu.SemaphoreType.DMA((2, most)),
            pltpu.SemaphoreType.DMA((2, most)),
            pltpu.VMEM((phases, buffer_rows, levels), F32),
            pltpu.VMEM((phases, buffer_rows, levels), F32),
            pltpu.VMEM((phases, 8, 2 * levels), F32),
            pltpu.VMEM((phases, count - 1, 8, 2 * levels), F32),
            pltpu.VMEM((rows + 2, wide, levels), F32),
            pltpu.VMEM((rows + 2, wide, levels), F32),
            pltpu.VMEM((wide, levels), F32),
            pltpu.VMEM((2, wide, levels), F32),
            pltpu.VMEM((2, rows + 2 * LEAD, levels), F32),
            pltpu.VMEM((cols, levels), F32),
            pltpu.VMEM((cols, levels), F32),
            pltpu.VMEM((8, levels), F32),
            pltpu.VMEM((8, levels), F32),
            pltpu.VMEM((levels, hidden), F32),
            pltpu.VMEM((STEPS, cols, hidden), BF16),
            pltpu.VMEM((STEPS, cols, hidden), F32),
            pltpu.VMEM((cols, in_width), BF16),
            pltpu.VMEM((STEPS, in_width, cols), BF16),
            pltpu.VMEM((2 * width + 2 * rim_rows, in_width), BF16),
            pltpu.VMEM((cols, hidden), F32),
            pltpu.VMEM((8, hidden), F32),
            pltpu.VMEM((cols, hidden), BF16),
            pltpu.VMEM((STEPS, 8, levels), F32),
            pltpu.SemaphoreType.DMA((phases, 8)),
            pltpu.SemaphoreType.DMA((phases, 8)),
            pltpu.SemaphoreType.DMA((phases,)),
            pltpu.SemaphoreType.DMA((phases,)),
        ],
        compiler_params=pltpu.CompilerParams(has_side_effects=True, collective_id=0, vmem_limit_bytes=44 * 1024 * 1024),
        name="chain",
    )(*[pltpu.with_memory_space_constraint(v, pltpu.HBM) for v in (initial_state, cotangent, w_in, b_in[None, :], w_out, edge_flips)])
    final, grad, gw_in, gb, gw_out = pl.pallas_call(
        functools.partial(finish_kernel, hidden),
        out_shape=(
            jax.ShapeDtypeStruct(initial_state.shape, F32),
            jax.ShapeDtypeStruct(initial_state.shape, F32),
            jax.ShapeDtypeStruct((in_width, hidden), F32),
            jax.ShapeDtypeStruct((chunks, LANES), F32),
            jax.ShapeDtypeStruct((levels, hidden), F32),
        ),
        in_specs=[vmem] * 4,
        out_specs=[hbm] * 5,
        scratch_shapes=[
            pltpu.VMEM((hidden // LANES, in_width, LANES), F32),
            pltpu.VMEM((levels, hidden), F32),
            pltpu.SemaphoreType.DMA((4 + hidden // LANES,)),
        ],
        compiler_params=pltpu.CompilerParams(vmem_limit_bytes=8 * 1024 * 1024),
        name="finish",
    )(final, grad, whole, gb)
    return (final, grad, gw_in, gb.reshape(hidden), gw_out)


def solution(mesh):
    in_specs = (P("tile", None, "sub"), P("tile", None, "sub"), P(), P(), P(), P("tile", None))
    out_specs = (P("tile", None, "sub"), P("tile", None, "sub"), P(), P(), P())
    body = functools.partial(shards, mesh.shape["tile"], mesh.shape["sub"])
    return jax.shard_map(body, mesh=mesh, in_specs=in_specs, out_specs=out_specs, check_vma=False)
```

```python
import functools

import jax
import jax.numpy as jnp
from jax import lax
from jax.experimental import pallas as pl
from jax.experimental.pallas import tpu as pltpu
from jax.sharding import PartitionSpec as P

STEPS = 4
TILE_ROW = 4
STEP_SIZE = 0.25
LEAD = 8
MESH = pl.DeviceIdType.MESH
F32 = jnp.float32
BF16 = jnp.bfloat16

LANES = 128


def layout(width, rows):
    names = [("NW", 1), ("NE", 1), ("SW", 1), ("SE", 1), ("N", width), ("S", width), ("W", rows), ("E", rows)]
    place, at = {}, 0
    for name, size in names:
        place[name] = (at, size)
        at += -(-size // 8) * 8
    return place, at


def reduce_plan(tiles, subs, flat_rows):
    sub_bits = [("sub", 1 << i) for i in range(subs.bit_length() - 1)]
    tile_bits = [("tile", 1 << i) for i in range(tiles.bit_length() - 1)]
    rest = sub_bits[1:] + tile_bits
    pairs = [tuple(rest[i:i + 2]) for i in range(0, len(rest), 2)]
    orders = [[tuple(sub_bits[:1])] + pairs, [tuple(sub_bits[:1])] + pairs[1:2] + pairs[:1] + pairs[2:]]
    unit = 8 * tiles * subs
    units = -(-flat_rows // unit)
    shares = [0, 0, 0, 0]
    for n, part in enumerate((0.3, 0.5, 0.8, 1.0)):
        shares[n] = int(round(units * part)) - sum(shares[:n])
    groups, at = [], 0
    for n, share in enumerate(shares):
        if share:
            groups.append((at, share * unit, orders[n % 2]))
            at += share * unit
    return groups, at


def dot(a, b, dims, precision=None):
    return lax.dot_general(a, b, (dims, ((), ())), preferred_element_type=F32, precision=precision)


def tree_sum(parts):
    while len(parts) > 1:
        parts = [parts[i] + parts[i + 1] if i + 1 < len(parts) else parts[i] for i in range(0, len(parts), 2)]
    return parts[0]


def chain_kernel(
    tiles, subs, rows, width, levels, hidden,
    state_hbm, cot_hbm, w_in_hbm, b_in_hbm, w_out_hbm, flips_hbm,
    final_ref, grad_ref, whole, gb_ref,
    state_ref, cot_ref, w_in_ref, b_in_ref, w_out_ref, flips_ref, load_sem,
    flat, out_half, in_half, red_ssem, red_rsem, gat_ssem, gat_rsem,
    gb_sum, gb_out, gb_in, gb_far, gb_ssem, gb_rsem,
    send, recv, sum_out, sum_in,
    padded, pad_grad, edge, lines, ends, field, gradient, totals, center, w_sum, hid, slope, patch, patch_t,
    rim, sides, w_side, pre, gp_sum, gp16, shifts,
    halo_ssem, halo_rsem, sum_ssem, sum_rsem,
):
    place, _ = layout(width, rows)
    cols = rows * width
    count = tiles * subs
    inv_total = 1.0 / (count * cols)
    me_t, me_s = lax.axis_index("tile"), lax.axis_index("sub")
    me = me_t * subs + me_s
    first, last = me_s == 0, me_s == subs - 1
    wide = width + 2 * LEAD
    in_width = w_in_ref.shape[0]
    stride = in_width + levels
    chunks = hidden // LANES
    groups, flat_rows = reduce_plan(tiles, subs, stride * chunks)
    unroll = count <= 64

    loads = [
        pltpu.make_async_copy(src, dst, load_sem.at[i])
        for i, (src, dst) in enumerate((
            (state_hbm, state_ref), (cot_hbm, cot_ref), (flips_hbm, flips_ref),
            (w_out_hbm, w_out_ref), (b_in_hbm, b_in_ref), (w_in_hbm, w_in_ref)))
    ]
    for load in loads:
        load.start()

    def device_at(by):
        other = lax.rem(me + by, count)
        return (other // subs, lax.rem(other, subs))

    barrier = pltpu.get_barrier_semaphore()

    def greet(by, carry):
        pl.semaphore_signal(barrier, inc=1, device_id=device_at(by), device_id_type=MESH)
        return carry

    lax.fori_loop(1, count, greet, 0, unroll=unroll)

    def tile_at(by):
        return lax.rem(me_t + by + 2 * tiles, tiles)

    def north_of(by):
        return (jnp.where(first, tile_at(by - TILE_ROW), tile_at(by)), jnp.where(first, subs - 1, me_s - 1))

    def south_of(by):
        return (jnp.where(last, tile_at(by + TILE_ROW), tile_at(by)), jnp.where(last, 0, me_s + 1))

    targets = {
        "N": north_of(0), "S": south_of(0), "W": (tile_at(-1), me_s), "E": (tile_at(1), me_s),
        "NW": north_of(-1), "NE": north_of(1), "SW": south_of(-1), "SE": south_of(1),
    }

    def halo_copies(p):
        out = []
        for i, (name, (at, size)) in enumerate(place.items()):
            out.append(pltpu.make_async_remote_copy(
                src_ref=send.at[p, pl.ds(at, size)], dst_ref=recv.at[p, pl.ds(at, size)],
                send_sem=halo_ssem.at[p, i], recv_sem=halo_rsem.at[p, i],
                device_id=targets[name], device_id_type=MESH))
        return out

    def start_halos(p):
        for copy in halo_copies(p):
            copy.start()

    def wait_halos(p, some=tuple(place)):
        for name, copy in zip(place, halo_copies(p)):
            if name in some:
                copy.wait()

    def start_sums(p, a, b):
        sum_out[p, 0:1] = jnp.concatenate([a, b], axis=1)

        def begin(by, carry):
            pltpu.make_async_remote_copy(
                src_ref=sum_out.at[p, pl.ds(0, 1)], dst_ref=sum_in.at[p, by - 1, pl.ds(0, 1)],
                send_sem=sum_ssem.at[p], recv_sem=sum_rsem.at[p],
                device_id=device_at(by), device_id_type=MESH).start()
            return carry

        lax.fori_loop(1, count, begin, 0, unroll=unroll)

    def wait_sums(p):
        pltpu.make_async_remote_copy(
            src_ref=sum_in.at[p, :, pl.ds(0, 1)], dst_ref=sum_in.at[p, :, pl.ds(0, 1)],
            send_sem=sum_ssem.at[p], recv_sem=sum_rsem.at[p],
            device_id=device_at(1), device_id_type=MESH).wait()
        if count <= 64:
            total = tree_sum([sum_out[p, 0:1]] + [sum_in[p, d, 0:1] for d in range(count - 1)])
        else:
            total = sum_out[p, 0:1] + jnp.sum(sum_in[p, :, 0:1], axis=0)
        return total[:, :levels], total[:, levels:]

    at_row = lax.broadcasted_iota(jnp.int32, (wide, wide), 0)
    at_col = lax.broadcasted_iota(jnp.int32, (wide, wide), 1)
    same = (at_row == at_col).astype(F32)
    turned = (at_row + at_col == wide - 1).astype(F32)
    diagonal = (
        lax.broadcasted_iota(jnp.int32, (levels, levels), 0) == lax.broadcasted_iota(jnp.int32, (levels, levels), 1)
    ).astype(F32)

    def column(flat_line):
        return jnp.sum(diagonal * flat_line, axis=1, keepdims=True)

    def turn_exact(turn, value):
        high = value.astype(BF16)
        left = value - high.astype(F32)
        middle = left.astype(BF16)
        low = (left - middle.astype(F32)).astype(BF16)
        parts = dot(turn.astype(BF16), jnp.concatenate([high, middle, low], axis=1), ((1,), (0,)))
        return parts[:, :levels] + parts[:, levels:2 * levels] + parts[:, 2 * levels:]

    def seam_matrix(mix):
        return turned * mix + same * (1.0 - mix)

    def send_field(p):
        for name, row in (("N", 0), ("S", rows - 1)):
            at = place[name][0]
            line = field[row * width:(row + 1) * width]
            send[p, at:at + width] = line
            for side, cell in (("W", 0), ("E", width - 1)):
                corner = place[name + side][0]
                send[p, corner:corner + 1] = line[cell:cell + 1]
        for name, cell in (("W", 0), ("E", width - 1)):
            at = place[name][0]
            for r in range(rows):
                send[p, at + r:at + r + 1] = field[r * width + cell:r * width + cell + 1]

    def gather_patch():
        for a in range(3):
            for b in range(3):
                o = 3 * a + b
                piece = padded[a:a + rows, LEAD - 1 + b:LEAD - 1 + b + width, :]
                patch[:, o * levels:(o + 1) * levels] = piece.reshape(cols, levels).astype(BF16)

    def add_lines(p, shift):
        for n, name in enumerate(("S", "N")):
            at = place[name][0]
            edge[LEAD:LEAD + width] = recv[p, at:at + width] - shift
            lines[n] = dot(turns[n].astype(BF16), edge[...].astype(BF16), ((1,), (0,)))
            for b in range(3):
                rim[n * width:(n + 1) * width, b * levels:(b + 1) * levels] = (
                    lines[n, LEAD - 1 + b:LEAD - 1 + b + width].astype(BF16))
            extra = dot(rim[n * width:(n + 1) * width], w_in_ref[6 * n * levels:(6 * n + 3) * levels], ((1,), (0,)))
            at = n * (cols - width)
            pre[at:at + width] += extra

    def add_sides(p, shift):
        def corner(name):
            at = place[name][0]
            return recv[p, at:at + 1] - shift

        for n, name in enumerate(("E", "W")):
            at = place[name][0]
            other = "WE"[n]
            ends[n, LEAD:LEAD + rows] = recv[p, at:at + rows] - shift
            ends[n, LEAD - 1:LEAD] = jnp.where(mixes[0] > 0.5, corner("S" + other), corner("S" + name))
            ends[n, LEAD + rows:LEAD + rows + 1] = jnp.where(mixes[1] > 0.5, corner("N" + other), corner("N" + name))
            for a in range(3):
                sides[n, 0:rows, a * levels:(a + 1) * levels] = (
                    ends[n, LEAD - 1 + a:LEAD - 1 + a + rows].astype(BF16))
            extra = dot(sides[n], w_side[n], ((1,), (0,)))
            for r in range(rows):
                at = r * width + n * (width - 1)
                pre[at:at + 1] += extra[r:r + 1]

    def whole_patch(k):
        for n, row in ((0, 0), (1, rows + 1)):
            padded[row] = lines[n]
        for n, cell in ((0, LEAD - 1), (1, LEAD + width)):
            for r in range(rows + 2):
                padded[r, cell:cell + 1] = ends[n, LEAD - 1 + r:LEAD + r]
        gather_patch()
        patch_t[k] = patch[...].T
        for row in (0, rows + 1):
            padded[row] = jnp.zeros((wide, levels), F32)
        for cell in (LEAD - 1, LEAD + width):
            padded[1:rows + 1, cell:cell + 1] = jnp.zeros((rows, 1, levels), F32)

    nothing = jnp.zeros((1, levels), F32)
    loads[0].wait()
    field[...] = state_ref[0].T
    send_field(0)
    pl.semaphore_wait(barrier, count - 1)
    start_halos(0)
    loads[1].wait()
    gradient[...] = cot_ref[0].T
    start_sums(0, nothing, jnp.sum(gradient[...], axis=0, keepdims=True))
    edge[...] = jnp.zeros_like(edge)
    padded[...] = jnp.zeros_like(padded)
    center[...] = jnp.zeros_like(center)
    totals[...] = jnp.zeros_like(totals)
    loads[2].wait()
    mixes = [
        jnp.where(first, flips_ref[0:1, 0:1], 0).astype(F32),
        jnp.where(last, flips_ref[0:1, 1:2], 0).astype(F32),
    ]
    turns = [seam_matrix(mix) for mix in mixes]
    flat[...] = jnp.zeros_like(flat)
    gb_sum[...] = jnp.zeros_like(gb_sum)
    ends[...] = jnp.zeros_like(ends)
    sides[...] = jnp.zeros_like(sides)
    for load in loads[3:]:
        load.wait()
    for n in range(2):
        for a in range(3):
            o = 3 * a + 2 * n
            w_side[n, a * levels:(a + 1) * levels] = w_in_ref[o * levels:(o + 1) * levels]
    w_sum[...] = w_in_ref[0:levels].astype(F32)
    for o in range(1, 9):
        w_sum[...] += w_in_ref[o * levels:(o + 1) * levels].astype(F32)

    def forward(k, carry):
        mid = center[0:1]
        padded[1:rows + 1, LEAD:LEAD + width, :] = (field[...] - mid).reshape(rows, width, levels)
        gather_patch()
        pre[...] = dot(patch[...], w_in_ref[...], ((1,), (0,)))
        wait_halos(k, ("N", "S"))
        add_lines(k, mid)
        wait_halos(k, ("W", "E", "NW", "NE", "SW", "SE"))
        add_sides(k, mid)
        sum_a, sum_b = wait_sums(k)
        shift = sum_a * (STEP_SIZE * inv_total)
        totals[1:2] += sum_b
        move = mid - shift
        shifts[k, 0:1] = move
        lift = b_in_ref[...] + jnp.sum(w_sum[...] * column(move), axis=0, keepdims=True)
        gp_sum[1:2] = lift
        act = pre[...] + lift
        low = (act * jax.nn.sigmoid(act)).astype(BF16)
        hid[k] = low
        tendency = dot(low, w_out_ref[...], ((1,), (1,)))
        field[...] = (field[...] - shift) + STEP_SIZE * tendency
        own = jnp.sum(tendency, axis=0, keepdims=True)

        @pl.when(k < STEPS - 1)
        def _():
            send_field(k + 1)
            start_halos(k + 1)
            start_sums(k + 1, own, nothing)

        center[0:1] = own * (STEP_SIZE / cols)
        center[1:2] = own
        value = pre[...] + gp_sum[1:2]
        sig = jax.nn.sigmoid(value)
        slope[k] = sig * (1.0 + value * (1.0 - sig))
        whole_patch(k)
        return carry

    lax.fori_loop(0, STEPS, forward, 0)

    def gradient_through(k, j):
        mid = jnp.sum(gradient[...], axis=0, keepdims=True) * (STEP_SIZE / cols)
        gh = dot((STEP_SIZE * gradient[...] - mid).astype(BF16), w_out_ref[...], ((1,), (0,)))

        @pl.when(j > 0)
        def _():
            sum_a, sum_b = wait_sums(STEPS + j - 1)
            totals[0:1] += sum_a
            totals[1:2] += sum_b

        level_grad = totals[1:2] * (STEP_SIZE * inv_total)
        lift = jnp.sum(w_out_ref[...].astype(F32) * column(mid - level_grad), axis=0, keepdims=True)
        gp = (gh + lift) * slope[k]
        gp16[...] = gp.astype(BF16)
        gp_sum[0:1] = jnp.sum(gp, axis=0, keepdims=True)
        return level_grad

    def spread(p, sums):
        gi = dot(gp16[...], w_in_ref[...], ((1,), (1,)))
        pad_grad[...] = jnp.zeros_like(pad_grad)
        if sums is not None:
            gi_sum = jnp.sum(gi, axis=0, keepdims=True)
            start_sums(p, sums, tree_sum([gi_sum[:, o * levels:(o + 1) * levels] for o in range(9)]))
        for a in range(3):
            for b in range(3):
                o = 3 * a + b
                piece = gi[:, o * levels:(o + 1) * levels].reshape(rows, width, levels)
                pad_grad[a:a + rows, LEAD - 1 + b:LEAD - 1 + b + width, :] += piece
        for n, (name, row) in enumerate((("N", 0), ("S", rows + 1))):
            at = place[name][0]
            edge[...] = turn_exact(turns[n], pad_grad[row])
            send[p, at:at + width] = edge[LEAD:LEAD + width]
            for side, cell in (("W", LEAD - 1), ("E", LEAD + width)):
                corner = place[name + side][0]
                send[p, corner:corner + 1] = edge[cell:cell + 1]
        for name, cell in (("W", LEAD - 1), ("E", LEAD + width)):
            at = place[name][0]
            for r in range(rows):
                send[p, at + r:at + r + 1] = pad_grad[r + 1, cell:cell + 1]
        start_halos(p)

    def keep():
        gradient[...] += pad_grad[1:rows + 1, LEAD:LEAD + width, :].reshape(cols, levels)

    def weigh(k, low_gt, c, many, shifted=True):
        lanes = slice(c * LANES, (c + many) * LANES)
        back = column(shifts[k, 0:1]) * gp_sum[0:1, lanes] if shifted else None
        gw = dot(patch_t[k], gp16[:, lanes], ((1,), (0,)))
        gw_out = dot(low_gt, hid[k, :, lanes], ((1,), (0,)))
        for n in range(many):
            at, part = (c + n) * stride, slice(n * LANES, (n + 1) * LANES)
            for o in range(9):
                grown = gw[o * levels:(o + 1) * levels, part]
                flat[at + o * levels:at + (o + 1) * levels] += grown + back[:, part] if shifted else grown
            flat[at + in_width:at + stride] += gw_out[:, part]

    def gradient_low(level_grad):
        return (STEP_SIZE * gradient[...] - level_grad).T.astype(BF16)

    def collect(p):
        for name, row in (("N", rows - 1), ("S", 0)):
            at = place[name][0]
            gradient[row * width:(row + 1) * width] += recv[p, at:at + width]
            for side, cell in (("W", width - 1), ("E", 0)):
                corner = place[name + side][0]
                gradient[row * width + cell:row * width + cell + 1] += recv[p, corner:corner + 1]
        for name, cell in (("W", width - 1), ("E", 0)):
            at = place[name][0]
            for r in range(rows):
                gradient[r * width + cell:r * width + cell + 1] += recv[p, at + r:at + r + 1]

    def backward(j, carry):
        k = STEPS - 1 - j
        p = STEPS + j
        level_grad = gradient_through(k, j)
        spread(p, jnp.where(j == 0, center[1:2], 0.0))
        low_gt = gradient_low(level_grad)
        keep()
        gb_sum[...] += gp_sum[0:1]
        weigh(k, low_gt, 0, chunks)
        wait_halos(p)
        collect(p)
        return carry

    lax.fori_loop(0, STEPS - 1, backward, 0)
    level_grad = gradient_through(0, STEPS - 1)
    low_gt = gradient_low(level_grad)

    def bit_of(bit):
        axis, step = bit
        return lax.rem((me_t if axis == "tile" else me_s) // step, 2)

    def peer_of(bits, mask):
        at = {"tile": me_t, "sub": me_s}
        for i, (axis, step) in enumerate(bits):
            if mask >> i & 1:
                at[axis] = at[axis] + step * (1 - 2 * bit_of((axis, step)))
        return (at["tile"], at["sub"])

    def place_of(bits, mask):
        index = 0
        for i, bit in enumerate(bits):
            index = index + (1 - bit_of(bit) if mask >> i & 1 else bit_of(bit)) * (1 << i)
        return index

    stages = []
    for start, size, order in groups:
        base, at, found = start, start, []
        for bits in order:
            piece = size >> len(bits)
            found.append((base, piece, at, bits))
            at += size - piece
            base = base + place_of(bits, 0) * piece
            size = piece
        stages.append((found, base, size))

    def rows_at(base, piece):
        return pl.ds(pl.multiple_of(base, 8), piece)

    def reduce_copies(g, i):
        base, piece, at, bits = stages[g][0][i]
        return [pltpu.make_async_remote_copy(
            src_ref=out_half.at[pl.ds(at + (m - 1) * piece, piece)],
            dst_ref=in_half.at[pl.ds(at + (m - 1) * piece, piece)],
            send_sem=red_ssem.at[g, i, m - 1], recv_sem=red_rsem.at[g, i, m - 1],
            device_id=peer_of(bits, m), device_id_type=MESH) for m in range(1, 1 << len(bits))]

    def reduce_start(g, i):
        base, piece, at, bits = stages[g][0][i]
        for m, copy in enumerate(reduce_copies(g, i), 1):
            away = flat[rows_at(base + place_of(bits, m) * piece, piece)]
            out_half[at + (m - 1) * piece:at + m * piece] = away.astype(BF16)
            copy.start()

    def reduce_wait(g, i):
        base, piece, at, bits = stages[g][0][i]
        own = rows_at(base + place_of(bits, 0) * piece, piece)
        total = flat[own]
        for m, copy in enumerate(reduce_copies(g, i), 1):
            copy.wait()
            total = total + in_half[at + (m - 1) * piece:at + m * piece].astype(F32)
        flat[own] = total

    def gather_copies(g, i):
        base, piece, at, bits = stages[g][0][i]
        own = rows_at(base + place_of(bits, 0) * piece, piece)
        return [pltpu.make_async_remote_copy(
            src_ref=whole.at[own], dst_ref=whole.at[own],
            send_sem=gat_ssem.at[g, i, m - 1], recv_sem=gat_rsem.at[g, i, m - 1],
            device_id=peer_of(bits, m), device_id_type=MESH) for m in range(1, 1 << len(bits))]

    near = tuple([("sub", 1 << i) for i in range(subs.bit_length() - 1)] + [("tile", 1)])
    far = tuple(("tile", 1 << i) for i in range(1, tiles.bit_length() - 1))

    def bias_copies(n):
        bits, source, slots = ((near, gb_out, gb_in), (far, gb_ref, gb_far))[n]
        return [pltpu.make_async_remote_copy(
            src_ref=source, dst_ref=slots.at[place_of(bits, 0)], send_sem=gb_ssem.at[n, m - 1], recv_sem=gb_rsem.at[n, m - 1],
            device_id=peer_of(bits, m), device_id_type=MESH) for m in range(1, 1 << len(bits))]

    def bias_start(n):
        bits, source, slots = ((near, gb_out, gb_in), (far, gb_ref, gb_far))[n]
        slots[place_of(bits, 0)] = source[...]
        for copy in bias_copies(n):
            copy.start()

    def bias_wait(n):
        for copy in bias_copies(n):
            copy.wait()
        slots = (gb_in, gb_far)[n]
        gb_ref[...] = tree_sum([slots[d] for d in range(slots.shape[0])])

    for c in range(chunks):
        lanes = slice(c * LANES, (c + 1) * LANES)
        gb_out[c:c + 1] = gb_sum[0:1, lanes] + gp_sum[0:1, lanes]
    bias_start(0)
    started = 0
    for c in range(0, chunks, 2):
        weigh(0, low_gt, c, 2, shifted=False)
        while started < len(groups) and (c + 2 == chunks or groups[started][0] + groups[started][1] <= (c + 2) * stride):
            reduce_start(started, 0)
            started += 1
    depth = max(len(order) for _, _, order in groups)
    for i in range(1, depth + 1):
        for g in range(len(groups)):
            reduce_wait(g, i - 1)
            if i < depth:
                reduce_start(g, i)
            else:
                _, base, size = stages[g]
                own = rows_at(base, size)
                whole[own] = flat[own].astype(BF16)
                for copy in gather_copies(g, depth - 1):
                    copy.start()
        if i == 1:
            spread(2 * STEPS - 1, None)
            keep()
            final_ref[0] = (field[...] - totals[0:1] * (STEP_SIZE * inv_total)).T
            bias_wait(0)
            bias_start(1)
        if i == 2:
            wait_halos(2 * STEPS - 1)
            collect(2 * STEPS - 1)
            grad_ref[0] = gradient[...].T
            bias_wait(1)
    for i in reversed(range(depth)):
        for g in range(len(groups)):
            for copy in gather_copies(g, i):
                copy.wait()
            if i > 0:
                for copy in gather_copies(g, i - 1):
                    copy.start()


def finish_kernel(hidden, final_in, grad_in, whole, gb_in, final_ref, grad_ref, gw_in_ref, gb_ref, gw_out_ref, wide_in, wide_out, sem):
    in_width, levels = gw_in_ref.shape[0], gw_out_ref.shape[0]
    stride = in_width + levels
    copies = [
        pltpu.make_async_copy(final_in, final_ref, sem.at[0]),
        pltpu.make_async_copy(grad_in, grad_ref, sem.at[1]),
        pltpu.make_async_copy(gb_in, gb_ref, sem.at[3]),
    ]
    for copy in copies:
        copy.start()
    for c in range(hidden // LANES):
        at, lanes = c * stride, slice(c * LANES, (c + 1) * LANES)
        wide_in[c] = whole[at:at + in_width].astype(F32)
        copies.append(pltpu.make_async_copy(wide_in.at[c], gw_in_ref.at[:, pl.ds(c * LANES, LANES)], sem.at[4 + c]))
        copies[-1].start()
        wide_out[:, lanes] = whole[at + in_width:at + stride].astype(F32)
    copies.append(pltpu.make_async_copy(wide_out, gw_out_ref, sem.at[2]))
    copies[-1].start()
    for copy in copies:
        copy.wait()


def shards(tiles, subs, initial_state, cotangent, w_in, b_in, w_out, edge_flips):
    _, levels, cols = initial_state.shape
    in_width, hidden = w_in.shape
    side = 1
    while side * side < cols * subs:
        side += 1
    rows, width = side // subs, side
    _, buffer_rows = layout(width, rows)
    phases = 2 * STEPS
    count = tiles * subs
    groups, flat_rows = reduce_plan(tiles, subs, (in_width + levels) * (hidden // LANES))
    depth = len(groups[0][2])
    chunks = hidden // LANES
    rim_rows = -(-rows // 16) * 16
    most = max(2 * subs, tiles // 2)
    wide = width + 2 * LEAD
    vmem = pl.BlockSpec(memory_space=pltpu.VMEM)
    hbm = pl.BlockSpec(memory_space=pltpu.HBM)
    final, grad, whole, gb = pl.pallas_call(
        functools.partial(chain_kernel, tiles, subs, rows, width, levels, hidden),
        out_shape=(
            jax.ShapeDtypeStruct(initial_state.shape, F32),
            jax.ShapeDtypeStruct(initial_state.shape, F32),
            jax.ShapeDtypeStruct((flat_rows, LANES), BF16),
            jax.ShapeDtypeStruct((chunks, LANES), F32),
        ),
        in_specs=[hbm] * 6,
        out_specs=[vmem] * 4,
        scratch_shapes=[
            pltpu.VMEM(initial_state.shape, F32),
            pltpu.VMEM(initial_state.shape, F32),
            pltpu.VMEM((in_width, hidden), BF16),
            pltpu.VMEM((1, hidden), F32),
            pltpu.VMEM((levels, hidden), BF16),
            pltpu.VMEM(edge_flips.shape, jnp.int32),
            pltpu.SemaphoreType.DMA((6,)),
            pltpu.VMEM((flat_rows, LANES), F32),
            pltpu.VMEM((flat_rows, LANES), BF16),
            pltpu.VMEM((flat_rows, LANES), BF16),
            pltpu.SemaphoreType.DMA((len(groups), depth, 3)),
            pltpu.SemaphoreType.DMA((len(groups), depth, 3)),
            pltpu.SemaphoreType.DMA((len(groups), depth, 3)),
            pltpu.SemaphoreType.DMA((len(groups), depth, 3)),
            pltpu.VMEM((1, hidden), F32),
            pltpu.VMEM((chunks, LANES), F32),
            pltpu.VMEM((2 * subs, chunks, LANES), F32),
            pltpu.VMEM((tiles // 2, chunks, LANES), F32),
            pltpu.SemaphoreType.DMA((2, most)),
            pltpu.SemaphoreType.DMA((2, most)),
            pltpu.VMEM((phases, buffer_rows, levels), F32),
            pltpu.VMEM((phases, buffer_rows, levels), F32),
            pltpu.VMEM((phases, 8, 2 * levels), F32),
            pltpu.VMEM((phases, count - 1, 8, 2 * levels), F32),
            pltpu.VMEM((rows + 2, wide, levels), F32),
            pltpu.VMEM((rows + 2, wide, levels), F32),
            pltpu.VMEM((wide, levels), F32),
            pltpu.VMEM((2, wide, levels), F32),
            pltpu.VMEM((2, rows + 2 * LEAD, levels), F32),
            pltpu.VMEM((cols, levels), F32),
            pltpu.VMEM((cols, levels), F32),
            pltpu.VMEM((8, levels), F32),
            pltpu.VMEM((8, levels), F32),
            pltpu.VMEM((levels, hidden), F32),
            pltpu.VMEM((STEPS, cols, hidden), BF16),
            pltpu.VMEM((STEPS, cols, hidden), F32),
            pltpu.VMEM((cols, in_width), BF16),
            pltpu.VMEM((STEPS, in_width, cols), BF16),
            pltpu.VMEM((2 * width, 3 * levels), BF16),
            pltpu.VMEM((2, rim_rows, 3 * levels), BF16),
            pltpu.VMEM((2, 3 * levels, hidden), BF16),
            pltpu.VMEM((cols, hidden), F32),
            pltpu.VMEM((8, hidden), F32),
            pltpu.VMEM((cols, hidden), BF16),
            pltpu.VMEM((STEPS, 8, levels), F32),
            pltpu.SemaphoreType.DMA((phases, 8)),
            pltpu.SemaphoreType.DMA((phases, 8)),
            pltpu.SemaphoreType.DMA((phases,)),
            pltpu.SemaphoreType.DMA((phases,)),
        ],
        compiler_params=pltpu.CompilerParams(has_side_effects=True, collective_id=0, vmem_limit_bytes=44 * 1024 * 1024),
        name="chain",
    )(*[pltpu.with_memory_space_constraint(v, pltpu.HBM) for v in (initial_state, cotangent, w_in, b_in[None, :], w_out, edge_flips)])
    final, grad, gw_in, gb, gw_out = pl.pallas_call(
        functools.partial(finish_kernel, hidden),
        out_shape=(
            jax.ShapeDtypeStruct(initial_state.shape, F32),
            jax.ShapeDtypeStruct(initial_state.shape, F32),
            jax.ShapeDtypeStruct((in_width, hidden), F32),
            jax.ShapeDtypeStruct((chunks, LANES), F32),
            jax.ShapeDtypeStruct((levels, hidden), F32),
        ),
        in_specs=[vmem] * 4,
        out_specs=[hbm] * 5,
        scratch_shapes=[
            pltpu.VMEM((hidden // LANES, in_width, LANES), F32),
            pltpu.VMEM((levels, hidden), F32),
            pltpu.SemaphoreType.DMA((4 + hidden // LANES,)),
        ],
        compiler_params=pltpu.CompilerParams(vmem_limit_bytes=8 * 1024 * 1024),
        name="finish",
    )(final, grad, whole, gb)
    return (final, grad, gw_in, gb.reshape(hidden), gw_out)


def solution(mesh):
    in_specs = (P("tile", None, "sub"), P("tile", None, "sub"), P(), P(), P(), P("tile", None))
    out_specs = (P("tile", None, "sub"), P("tile", None, "sub"), P(), P(), P())
    body = functools.partial(shards, mesh.shape["tile"], mesh.shape["sub"])
    return jax.shard_map(body, mesh=mesh, in_specs=in_specs, out_specs=out_specs, check_vma=False)
```

```python
import functools

import jax
import jax.numpy as jnp
from jax import lax
from jax.experimental import pallas as pl
from jax.experimental.pallas import tpu as pltpu
from jax.sharding import PartitionSpec as P

STEPS = 4
TILE_ROW = 4
STEP_SIZE = 0.25
LEAD = 8
MESH = pl.DeviceIdType.MESH
F32 = jnp.float32
BF16 = jnp.bfloat16

LANES = 128


def layout(width, rows):
    names = [("NW", 1), ("NE", 1), ("SW", 1), ("SE", 1), ("N", width), ("S", width), ("W", rows), ("E", rows)]
    place, at = {}, 0
    for name, size in names:
        place[name] = (at, size)
        at += -(-size // 8) * 8
    return place, at


def reduce_plan(tiles, subs, flat_rows):
    sub_bits = [("sub", 1 << i) for i in range(subs.bit_length() - 1)]
    tile_bits = [("tile", 1 << i) for i in range(tiles.bit_length() - 1)]
    rest = sub_bits[1:] + tile_bits
    pairs = [tuple(rest[i:i + 2]) for i in range(0, len(rest), 2)]
    orders = [[tuple(sub_bits[:1])] + pairs, [tuple(sub_bits[:1])] + pairs[1:2] + pairs[:1] + pairs[2:]]
    unit = 8 * tiles * subs
    units = -(-flat_rows // unit)
    shares = [0, 0, 0, 0]
    for n, part in enumerate((0.3, 0.5, 0.8, 1.0)):
        shares[n] = int(round(units * part)) - sum(shares[:n])
    groups, at = [], 0
    for n, share in enumerate(shares):
        if share:
            groups.append((at, share * unit, orders[n % 2]))
            at += share * unit
    return groups, at


def dot(a, b, dims, precision=None):
    return lax.dot_general(a, b, (dims, ((), ())), preferred_element_type=F32, precision=precision)


def tree_sum(parts):
    while len(parts) > 1:
        parts = [parts[i] + parts[i + 1] if i + 1 < len(parts) else parts[i] for i in range(0, len(parts), 2)]
    return parts[0]


def chain_kernel(
    tiles, subs, rows, width, levels, hidden,
    state_hbm, cot_hbm, w_in_hbm, b_in_hbm, w_out_hbm, flips_hbm,
    final_ref, grad_ref, whole, gb_ref,
    state_ref, cot_ref, w_in_ref, b_in_ref, w_out_ref, flips_ref, load_sem,
    flat, out_half, in_half, red_ssem, red_rsem, gat_ssem, gat_rsem,
    gb_sum, gb_out, gb_in, gb_far, gb_ssem, gb_rsem,
    send, recv, sum_out, sum_in,
    padded, pad_grad, edge, lines, ends, field, gradient, totals, center, w_sum, hid, slope, patch, patch_t,
    rim, sides, w_side, pre, gp_sum, gp16, shifts,
    halo_ssem, halo_rsem, sum_ssem, sum_rsem,
):
    place, _ = layout(width, rows)
    cols = rows * width
    count = tiles * subs
    inv_total = 1.0 / (count * cols)
    me_t, me_s = lax.axis_index("tile"), lax.axis_index("sub")
    me = me_t * subs + me_s
    first, last = me_s == 0, me_s == subs - 1
    wide = width + 2 * LEAD
    in_width = w_in_ref.shape[0]
    stride = in_width + levels
    chunks = hidden // LANES
    groups, flat_rows = reduce_plan(tiles, subs, stride * chunks)
    unroll = count <= 64

    loads = [
        pltpu.make_async_copy(src, dst, load_sem.at[i])
        for i, (src, dst) in enumerate((
            (state_hbm, state_ref), (cot_hbm, cot_ref), (flips_hbm, flips_ref),
            (w_out_hbm, w_out_ref), (b_in_hbm, b_in_ref), (w_in_hbm, w_in_ref)))
    ]
    for load in loads:
        load.start()

    def device_at(by):
        other = lax.rem(me + by, count)
        return (other // subs, lax.rem(other, subs))

    barrier = pltpu.get_barrier_semaphore()

    def greet(by, carry):
        pl.semaphore_signal(barrier, inc=1, device_id=device_at(by), device_id_type=MESH)
        return carry

    lax.fori_loop(1, count, greet, 0, unroll=unroll)

    def tile_at(by):
        return lax.rem(me_t + by + 2 * tiles, tiles)

    def north_of(by):
        return (jnp.where(first, tile_at(by - TILE_ROW), tile_at(by)), jnp.where(first, subs - 1, me_s - 1))

    def south_of(by):
        return (jnp.where(last, tile_at(by + TILE_ROW), tile_at(by)), jnp.where(last, 0, me_s + 1))

    targets = {
        "N": north_of(0), "S": south_of(0), "W": (tile_at(-1), me_s), "E": (tile_at(1), me_s),
        "NW": north_of(-1), "NE": north_of(1), "SW": south_of(-1), "SE": south_of(1),
    }

    def halo_copies(p):
        out = []
        for i, (name, (at, size)) in enumerate(place.items()):
            out.append(pltpu.make_async_remote_copy(
                src_ref=send.at[p, pl.ds(at, size)], dst_ref=recv.at[p, pl.ds(at, size)],
                send_sem=halo_ssem.at[p, i], recv_sem=halo_rsem.at[p, i],
                device_id=targets[name], device_id_type=MESH))
        return out

    def start_halos(p):
        for copy in halo_copies(p):
            copy.start()

    def wait_halos(p, some=tuple(place)):
        for name, copy in zip(place, halo_copies(p)):
            if name in some:
                copy.wait()

    def start_sums(p, a, b):
        sum_out[p, 0:1] = jnp.concatenate([a, b], axis=1)

        def begin(by, carry):
            pltpu.make_async_remote_copy(
                src_ref=sum_out.at[p, pl.ds(0, 1)], dst_ref=sum_in.at[p, by - 1, pl.ds(0, 1)],
                send_sem=sum_ssem.at[p], recv_sem=sum_rsem.at[p],
                device_id=device_at(by), device_id_type=MESH).start()
            return carry

        lax.fori_loop(1, count, begin, 0, unroll=unroll)

    def wait_sums(p):
        pltpu.make_async_remote_copy(
            src_ref=sum_in.at[p, :, pl.ds(0, 1)], dst_ref=sum_in.at[p, :, pl.ds(0, 1)],
            send_sem=sum_ssem.at[p], recv_sem=sum_rsem.at[p],
            device_id=device_at(1), device_id_type=MESH).wait()
        if count <= 64:
            total = tree_sum([sum_out[p, 0:1]] + [sum_in[p, d, 0:1] for d in range(count - 1)])
        else:
            total = sum_out[p, 0:1] + jnp.sum(sum_in[p, :, 0:1], axis=0)
        return total[:, :levels], total[:, levels:]

    at_row = lax.broadcasted_iota(jnp.int32, (wide, wide), 0)
    at_col = lax.broadcasted_iota(jnp.int32, (wide, wide), 1)
    same = (at_row == at_col).astype(F32)
    turned = (at_row + at_col == wide - 1).astype(F32)
    diagonal = (
        lax.broadcasted_iota(jnp.int32, (levels, levels), 0) == lax.broadcasted_iota(jnp.int32, (levels, levels), 1)
    ).astype(F32)

    def column(flat_line):
        return jnp.sum(diagonal * flat_line, axis=1, keepdims=True)

    def turn_exact(turn, value):
        high = value.astype(BF16)
        left = value - high.astype(F32)
        middle = left.astype(BF16)
        low = (left - middle.astype(F32)).astype(BF16)
        parts = dot(turn.astype(BF16), jnp.concatenate([high, middle, low], axis=1), ((1,), (0,)))
        return parts[:, :levels] + parts[:, levels:2 * levels] + parts[:, 2 * levels:]

    def seam_matrix(mix):
        return turned * mix + same * (1.0 - mix)

    def send_field(p):
        for name, row in (("N", 0), ("S", rows - 1)):
            at = place[name][0]
            line = field[row * width:(row + 1) * width]
            send[p, at:at + width] = line
            for side, cell in (("W", 0), ("E", width - 1)):
                corner = place[name + side][0]
                send[p, corner:corner + 1] = line[cell:cell + 1]
        for name, cell in (("W", 0), ("E", width - 1)):
            at = place[name][0]
            for r in range(rows):
                send[p, at + r:at + r + 1] = field[r * width + cell:r * width + cell + 1]

    def gather_patch():
        for a in range(3):
            for b in range(3):
                o = 3 * a + b
                piece = padded[a:a + rows, LEAD - 1 + b:LEAD - 1 + b + width, :]
                patch[:, o * levels:(o + 1) * levels] = piece.reshape(cols, levels).astype(BF16)

    def add_lines(p, shift):
        for n, name in enumerate(("S", "N")):
            at = place[name][0]
            edge[LEAD:LEAD + width] = recv[p, at:at + width] - shift
            lines[n] = dot(turns[n].astype(BF16), edge[...].astype(BF16), ((1,), (0,)))
            for b in range(3):
                rim[n * width:(n + 1) * width, b * levels:(b + 1) * levels] = (
                    lines[n, LEAD - 1 + b:LEAD - 1 + b + width].astype(BF16))
            extra = dot(rim[n * width:(n + 1) * width], w_in_ref[6 * n * levels:(6 * n + 3) * levels], ((1,), (0,)))
            at = n * (cols - width)
            pre[at:at + width] += extra

    def add_sides(p, shift):
        def corner(name):
            at = place[name][0]
            return recv[p, at:at + 1] - shift

        for n, name in enumerate(("E", "W")):
            at = place[name][0]
            other = "WE"[n]
            ends[n, LEAD:LEAD + rows] = recv[p, at:at + rows] - shift
            ends[n, LEAD - 1:LEAD] = jnp.where(mixes[0] > 0.5, corner("S" + other), corner("S" + name))
            ends[n, LEAD + rows:LEAD + rows + 1] = jnp.where(mixes[1] > 0.5, corner("N" + other), corner("N" + name))
            for a in range(3):
                sides[n, 0:rows, a * levels:(a + 1) * levels] = (
                    ends[n, LEAD - 1 + a:LEAD - 1 + a + rows].astype(BF16))
            extra = dot(sides[n], w_side[n], ((1,), (0,)))
            for r in range(rows):
                at = r * width + n * (width - 1)
                pre[at:at + 1] += extra[r:r + 1]

    def whole_patch(k):
        for n, row in ((0, 0), (1, rows + 1)):
            padded[row] = lines[n]
        for n, cell in ((0, LEAD - 1), (1, LEAD + width)):
            for r in range(rows + 2):
                padded[r, cell:cell + 1] = ends[n, LEAD - 1 + r:LEAD + r]
        gather_patch()
        patch_t[k] = patch[...].T
        for row in (0, rows + 1):
            padded[row] = jnp.zeros((wide, levels), F32)
        for cell in (LEAD - 1, LEAD + width):
            padded[1:rows + 1, cell:cell + 1] = jnp.zeros((rows, 1, levels), F32)

    nothing = jnp.zeros((1, levels), F32)
    loads[0].wait()
    field[...] = state_ref[0].T
    send_field(0)
    pl.semaphore_wait(barrier, count - 1)
    start_halos(0)
    loads[1].wait()
    gradient[...] = cot_ref[0].T
    start_sums(0, nothing, jnp.sum(gradient[...], axis=0, keepdims=True))
    edge[...] = jnp.zeros_like(edge)
    padded[...] = jnp.zeros_like(padded)
    center[...] = jnp.zeros_like(center)
    totals[...] = jnp.zeros_like(totals)
    loads[2].wait()
    mixes = [
        jnp.where(first, flips_ref[0:1, 0:1], 0).astype(F32),
        jnp.where(last, flips_ref[0:1, 1:2], 0).astype(F32),
    ]
    turns = [seam_matrix(mix) for mix in mixes]
    flat[...] = jnp.zeros_like(flat)
    gb_sum[...] = jnp.zeros_like(gb_sum)
    ends[...] = jnp.zeros_like(ends)
    sides[...] = jnp.zeros_like(sides)
    for load in loads[3:]:
        load.wait()
    for n in range(2):
        for a in range(3):
            o = 3 * a + 2 * n
            w_side[n, a * levels:(a + 1) * levels] = w_in_ref[o * levels:(o + 1) * levels]
    w_sum[...] = w_in_ref[0:levels].astype(F32)
    for o in range(1, 9):
        w_sum[...] += w_in_ref[o * levels:(o + 1) * levels].astype(F32)

    def forward(k, carry):
        mid = center[0:1]
        padded[1:rows + 1, LEAD:LEAD + width, :] = (field[...] - mid).reshape(rows, width, levels)
        gather_patch()
        pre[...] = dot(patch[...], w_in_ref[...], ((1,), (0,)))
        wait_halos(k, ("N", "S"))
        add_lines(k, mid)
        wait_halos(k, ("W", "E", "NW", "NE", "SW", "SE"))
        add_sides(k, mid)
        sum_a, sum_b = wait_sums(k)
        shift = sum_a * (STEP_SIZE * inv_total)
        totals[1:2] += sum_b
        move = mid - shift
        shifts[k, 0:1] = move
        lift = b_in_ref[...] + jnp.sum(w_sum[...] * column(move), axis=0, keepdims=True)
        gp_sum[1:2] = lift
        act = pre[...] + lift
        low = (act * jax.nn.sigmoid(act)).astype(BF16)
        hid[k] = low
        tendency = dot(low, w_out_ref[...], ((1,), (1,)))
        field[...] = (field[...] - shift) + STEP_SIZE * tendency
        own = jnp.sum(tendency, axis=0, keepdims=True)

        @pl.when(k < STEPS - 1)
        def _():
            send_field(k + 1)
            start_halos(k + 1)
            start_sums(k + 1, own, nothing)

        center[0:1] = own * (STEP_SIZE / cols)
        center[1:2] = own
        value = pre[...] + gp_sum[1:2]
        sig = jax.nn.sigmoid(value)
        slope[k] = sig * (1.0 + value * (1.0 - sig))
        whole_patch(k)
        return carry

    lax.fori_loop(0, STEPS, forward, 0)

    def gradient_through(k, j):
        mid = jnp.sum(gradient[...], axis=0, keepdims=True) * (STEP_SIZE / cols)
        gh = dot((STEP_SIZE * gradient[...] - mid).astype(BF16), w_out_ref[...], ((1,), (0,)))

        @pl.when(j > 0)
        def _():
            sum_a, sum_b = wait_sums(STEPS + j - 1)
            totals[0:1] += sum_a
            totals[1:2] += sum_b

        level_grad = totals[1:2] * (STEP_SIZE * inv_total)
        lift = jnp.sum(w_out_ref[...].astype(F32) * column(mid - level_grad), axis=0, keepdims=True)
        gp = (gh + lift) * slope[k]
        gp16[...] = gp.astype(BF16)
        gp_sum[0:1] = jnp.sum(gp, axis=0, keepdims=True)
        return level_grad

    def spread(p, sums):
        gi = dot(gp16[...], w_in_ref[...], ((1,), (1,)))
        pad_grad[...] = jnp.zeros_like(pad_grad)
        if sums is not None:
            gi_sum = jnp.sum(gi, axis=0, keepdims=True)
            start_sums(p, sums, tree_sum([gi_sum[:, o * levels:(o + 1) * levels] for o in range(9)]))
        for a in range(3):
            for b in range(3):
                o = 3 * a + b
                piece = gi[:, o * levels:(o + 1) * levels].reshape(rows, width, levels)
                pad_grad[a:a + rows, LEAD - 1 + b:LEAD - 1 + b + width, :] += piece
        for n, (name, row) in enumerate((("N", 0), ("S", rows + 1))):
            at = place[name][0]
            edge[...] = turn_exact(turns[n], pad_grad[row])
            send[p, at:at + width] = edge[LEAD:LEAD + width]
            for side, cell in (("W", LEAD - 1), ("E", LEAD + width)):
                corner = place[name + side][0]
                send[p, corner:corner + 1] = edge[cell:cell + 1]
        for name, cell in (("W", LEAD - 1), ("E", LEAD + width)):
            at = place[name][0]
            for r in range(rows):
                send[p, at + r:at + r + 1] = pad_grad[r + 1, cell:cell + 1]
        start_halos(p)

    def keep():
        gradient[...] += pad_grad[1:rows + 1, LEAD:LEAD + width, :].reshape(cols, levels)

    def weigh(k, low_gt, c, many, shifted=True):
        lanes = slice(c * LANES, (c + many) * LANES)
        back = column(shifts[k, 0:1]) * gp_sum[0:1, lanes] if shifted else None
        gw = dot(patch_t[k], gp16[:, lanes], ((1,), (0,)))
        gw_out = dot(low_gt, hid[k, :, lanes], ((1,), (0,)))
        for n in range(many):
            at, part = (c + n) * stride, slice(n * LANES, (n + 1) * LANES)
            for o in range(9):
                grown = gw[o * levels:(o + 1) * levels, part]
                flat[at + o * levels:at + (o + 1) * levels] += grown + back[:, part] if shifted else grown
            flat[at + in_width:at + stride] += gw_out[:, part]

    def gradient_low(level_grad):
        return (STEP_SIZE * gradient[...] - level_grad).T.astype(BF16)

    def collect(p):
        for name, row in (("N", rows - 1), ("S", 0)):
            at = place[name][0]
            gradient[row * width:(row + 1) * width] += recv[p, at:at + width]
            for side, cell in (("W", width - 1), ("E", 0)):
                corner = place[name + side][0]
                gradient[row * width + cell:row * width + cell + 1] += recv[p, corner:corner + 1]
        for name, cell in (("W", width - 1), ("E", 0)):
            at = place[name][0]
            for r in range(rows):
                gradient[r * width + cell:r * width + cell + 1] += recv[p, at + r:at + r + 1]

    def backward(j, carry):
        k = STEPS - 1 - j
        p = STEPS + j
        level_grad = gradient_through(k, j)
        spread(p, jnp.where(j == 0, center[1:2], 0.0))
        low_gt = gradient_low(level_grad)
        keep()
        gb_sum[...] += gp_sum[0:1]
        weigh(k, low_gt, 0, chunks)
        wait_halos(p)
        collect(p)
        return carry

    lax.fori_loop(0, STEPS - 1, backward, 0)
    level_grad = gradient_through(0, STEPS - 1)
    low_gt = gradient_low(level_grad)

    def bit_of(bit):
        axis, step = bit
        return lax.rem((me_t if axis == "tile" else me_s) // step, 2)

    def peer_of(bits, mask):
        at = {"tile": me_t, "sub": me_s}
        for i, (axis, step) in enumerate(bits):
            if mask >> i & 1:
                at[axis] = at[axis] + step * (1 - 2 * bit_of((axis, step)))
        return (at["tile"], at["sub"])

    def place_of(bits, mask):
        index = 0
        for i, bit in enumerate(bits):
            index = index + (1 - bit_of(bit) if mask >> i & 1 else bit_of(bit)) * (1 << i)
        return index

    stages = []
    for start, size, order in groups:
        base, at, found = start, start, []
        for bits in order:
            piece = size >> len(bits)
            found.append((base, piece, at, bits))
            at += size - piece
            base = base + place_of(bits, 0) * piece
            size = piece
        stages.append((found, base, size))

    def rows_at(base, piece):
        return pl.ds(pl.multiple_of(base, 8), piece)

    def reduce_copies(g, i):
        base, piece, at, bits = stages[g][0][i]
        return [pltpu.make_async_remote_copy(
            src_ref=out_half.at[pl.ds(at + (m - 1) * piece, piece)],
            dst_ref=in_half.at[pl.ds(at + (m - 1) * piece, piece)],
            send_sem=red_ssem.at[g, i, m - 1], recv_sem=red_rsem.at[g, i, m - 1],
            device_id=peer_of(bits, m), device_id_type=MESH) for m in range(1, 1 << len(bits))]

    def reduce_start(g, i):
        base, piece, at, bits = stages[g][0][i]
        for m, copy in reversed(list(enumerate(reduce_copies(g, i), 1))):
            away = flat[rows_at(base + place_of(bits, m) * piece, piece)]
            out_half[at + (m - 1) * piece:at + m * piece] = away.astype(BF16)
            copy.start()

    def reduce_wait(g, i):
        base, piece, at, bits = stages[g][0][i]
        own = rows_at(base + place_of(bits, 0) * piece, piece)
        total = flat[own]
        for m, copy in enumerate(reduce_copies(g, i), 1):
            copy.wait()
            total = total + in_half[at + (m - 1) * piece:at + m * piece].astype(F32)
        flat[own] = total

    def gather_copies(g, i):
        base, piece, at, bits = stages[g][0][i]
        own = rows_at(base + place_of(bits, 0) * piece, piece)
        return [pltpu.make_async_remote_copy(
            src_ref=whole.at[own], dst_ref=whole.at[own],
            send_sem=gat_ssem.at[g, i, m - 1], recv_sem=gat_rsem.at[g, i, m - 1],
            device_id=peer_of(bits, m), device_id_type=MESH) for m in range(1, 1 << len(bits))]

    near = tuple([("sub", 1 << i) for i in range(subs.bit_length() - 1)] + [("tile", 1)])
    far = tuple(("tile", 1 << i) for i in range(1, tiles.bit_length() - 1))

    def bias_copies(n):
        bits, source, slots = ((near, gb_out, gb_in), (far, gb_ref, gb_far))[n]
        return [pltpu.make_async_remote_copy(
            src_ref=source, dst_ref=slots.at[place_of(bits, 0)], send_sem=gb_ssem.at[n, m - 1], recv_sem=gb_rsem.at[n, m - 1],
            device_id=peer_of(bits, m), device_id_type=MESH) for m in range(1, 1 << len(bits))]

    def bias_start(n):
        bits, source, slots = ((near, gb_out, gb_in), (far, gb_ref, gb_far))[n]
        slots[place_of(bits, 0)] = source[...]
        for copy in bias_copies(n):
            copy.start()

    def bias_wait(n):
        for copy in bias_copies(n):
            copy.wait()
        slots = (gb_in, gb_far)[n]
        gb_ref[...] = tree_sum([slots[d] for d in range(slots.shape[0])])

    for c in range(chunks):
        lanes = slice(c * LANES, (c + 1) * LANES)
        gb_out[c:c + 1] = gb_sum[0:1, lanes] + gp_sum[0:1, lanes]
    bias_start(0)
    started = 0
    for c in range(0, chunks, 2):
        weigh(0, low_gt, c, 2, shifted=False)
        while started < len(groups) and (c + 2 == chunks or groups[started][0] + groups[started][1] <= (c + 2) * stride):
            reduce_start(started, 0)
            started += 1
    depth = max(len(order) for _, _, order in groups)
    for i in range(1, depth + 1):
        for g in range(len(groups)):
            reduce_wait(g, i - 1)
            if i < depth:
                reduce_start(g, i)
            else:
                _, base, size = stages[g]
                own = rows_at(base, size)
                whole[own] = flat[own].astype(BF16)
                for copy in reversed(gather_copies(g, depth - 1)):
                    copy.start()
        if i == 1:
            spread(2 * STEPS - 1, None)
            keep()
            final_ref[0] = (field[...] - totals[0:1] * (STEP_SIZE * inv_total)).T
            bias_wait(0)
            bias_start(1)
        if i == 2:
            wait_halos(2 * STEPS - 1)
            collect(2 * STEPS - 1)
            grad_ref[0] = gradient[...].T
            bias_wait(1)
    for i in reversed(range(depth)):
        for g in range(len(groups)):
            for copy in gather_copies(g, i):
                copy.wait()
            if i > 0:
                for copy in reversed(gather_copies(g, i - 1)):
                    copy.start()


def finish_kernel(hidden, final_in, grad_in, whole, gb_in, final_ref, grad_ref, gw_in_ref, gb_ref, gw_out_ref, wide_in, wide_out, sem):
    in_width, levels = gw_in_ref.shape[0], gw_out_ref.shape[0]
    stride = in_width + levels
    copies = [
        pltpu.make_async_copy(final_in, final_ref, sem.at[0]),
        pltpu.make_async_copy(grad_in, grad_ref, sem.at[1]),
        pltpu.make_async_copy(gb_in, gb_ref, sem.at[3]),
    ]
    for copy in copies:
        copy.start()
    for c in range(hidden // LANES):
        at, lanes = c * stride, slice(c * LANES, (c + 1) * LANES)
        wide_in[c] = whole[at:at + in_width].astype(F32)
        copies.append(pltpu.make_async_copy(wide_in.at[c], gw_in_ref.at[:, pl.ds(c * LANES, LANES)], sem.at[4 + c]))
        copies[-1].start()
        wide_out[:, lanes] = whole[at + in_width:at + stride].astype(F32)
    copies.append(pltpu.make_async_copy(wide_out, gw_out_ref, sem.at[2]))
    copies[-1].start()
    for copy in copies:
        copy.wait()


def shards(tiles, subs, initial_state, cotangent, w_in, b_in, w_out, edge_flips):
    _, levels, cols = initial_state.shape
    in_width, hidden = w_in.shape
    side = 1
    while side * side < cols * subs:
        side += 1
    rows, width = side // subs, side
    _, buffer_rows = layout(width, rows)
    phases = 2 * STEPS
    count = tiles * subs
    groups, flat_rows = reduce_plan(tiles, subs, (in_width + levels) * (hidden // LANES))
    depth = len(groups[0][2])
    chunks = hidden // LANES
    rim_rows = -(-rows // 16) * 16
    most = max(2 * subs, tiles // 2)
    wide = width + 2 * LEAD
    vmem = pl.BlockSpec(memory_space=pltpu.VMEM)
    hbm = pl.BlockSpec(memory_space=pltpu.HBM)
    final, grad, whole, gb = pl.pallas_call(
        functools.partial(chain_kernel, tiles, subs, rows, width, levels, hidden),
        out_shape=(
            jax.ShapeDtypeStruct(initial_state.shape, F32),
            jax.ShapeDtypeStruct(initial_state.shape, F32),
            jax.ShapeDtypeStruct((flat_rows, LANES), BF16),
            jax.ShapeDtypeStruct((chunks, LANES), F32),
        ),
        in_specs=[hbm] * 6,
        out_specs=[vmem] * 4,
        scratch_shapes=[
            pltpu.VMEM(initial_state.shape, F32),
            pltpu.VMEM(initial_state.shape, F32),
            pltpu.VMEM((in_width, hidden), BF16),
            pltpu.VMEM((1, hidden), F32),
            pltpu.VMEM((levels, hidden), BF16),
            pltpu.VMEM(edge_flips.shape, jnp.int32),
            pltpu.SemaphoreType.DMA((6,)),
            pltpu.VMEM((flat_rows, LANES), F32),
            pltpu.VMEM((flat_rows, LANES), BF16),
            pltpu.VMEM((flat_rows, LANES), BF16),
            pltpu.SemaphoreType.DMA((len(groups), depth, 3)),
            pltpu.SemaphoreType.DMA((len(groups), depth, 3)),
            pltpu.SemaphoreType.DMA((len(groups), depth, 3)),
            pltpu.SemaphoreType.DMA((len(groups), depth, 3)),
            pltpu.VMEM((1, hidden), F32),
            pltpu.VMEM((chunks, LANES), F32),
            pltpu.VMEM((2 * subs, chunks, LANES), F32),
            pltpu.VMEM((tiles // 2, chunks, LANES), F32),
            pltpu.SemaphoreType.DMA((2, most)),
            pltpu.SemaphoreType.DMA((2, most)),
            pltpu.VMEM((phases, buffer_rows, levels), F32),
            pltpu.VMEM((phases, buffer_rows, levels), F32),
            pltpu.VMEM((phases, 8, 2 * levels), F32),
            pltpu.VMEM((phases, count - 1, 8, 2 * levels), F32),
            pltpu.VMEM((rows + 2, wide, levels), F32),
            pltpu.VMEM((rows + 2, wide, levels), F32),
            pltpu.VMEM((wide, levels), F32),
            pltpu.VMEM((2, wide, levels), F32),
            pltpu.VMEM((2, rows + 2 * LEAD, levels), F32),
            pltpu.VMEM((cols, levels), F32),
            pltpu.VMEM((cols, levels), F32),
            pltpu.VMEM((8, levels), F32),
            pltpu.VMEM((8, levels), F32),
            pltpu.VMEM((levels, hidden), F32),
            pltpu.VMEM((STEPS, cols, hidden), BF16),
            pltpu.VMEM((STEPS, cols, hidden), F32),
            pltpu.VMEM((cols, in_width), BF16),
            pltpu.VMEM((STEPS, in_width, cols), BF16),
            pltpu.VMEM((2 * width, 3 * levels), BF16),
            pltpu.VMEM((2, rim_rows, 3 * levels), BF16),
            pltpu.VMEM((2, 3 * levels, hidden), BF16),
            pltpu.VMEM((cols, hidden), F32),
            pltpu.VMEM((8, hidden), F32),
            pltpu.VMEM((cols, hidden), BF16),
            pltpu.VMEM((STEPS, 8, levels), F32),
            pltpu.SemaphoreType.DMA((phases, 8)),
            pltpu.SemaphoreType.DMA((phases, 8)),
            pltpu.SemaphoreType.DMA((phases,)),
            pltpu.SemaphoreType.DMA((phases,)),
        ],
        compiler_params=pltpu.CompilerParams(has_side_effects=True, collective_id=0, vmem_limit_bytes=44 * 1024 * 1024),
        name="chain",
    )(*[pltpu.with_memory_space_constraint(v, pltpu.HBM) for v in (initial_state, cotangent, w_in, b_in[None, :], w_out, edge_flips)])
    final, grad, gw_in, gb, gw_out = pl.pallas_call(
        functools.partial(finish_kernel, hidden),
        out_shape=(
            jax.ShapeDtypeStruct(initial_state.shape, F32),
            jax.ShapeDtypeStruct(initial_state.shape, F32),
            jax.ShapeDtypeStruct((in_width, hidden), F32),
            jax.ShapeDtypeStruct((chunks, LANES), F32),
            jax.ShapeDtypeStruct((levels, hidden), F32),
        ),
        in_specs=[vmem] * 4,
        out_specs=[hbm] * 5,
        scratch_shapes=[
            pltpu.VMEM((hidden // LANES, in_width, LANES), F32),
            pltpu.VMEM((levels, hidden), F32),
            pltpu.SemaphoreType.DMA((4 + hidden // LANES,)),
        ],
        compiler_params=pltpu.CompilerParams(vmem_limit_bytes=8 * 1024 * 1024),
        name="finish",
    )(final, grad, whole, gb)
    return (final, grad, gw_in, gb.reshape(hidden), gw_out)


def solution(mesh):
    in_specs = (P("tile", None, "sub"), P("tile", None, "sub"), P(), P(), P(), P("tile", None))
    out_specs = (P("tile", None, "sub"), P("tile", None, "sub"), P(), P(), P())
    body = functools.partial(shards, mesh.shape["tile"], mesh.shape["sub"])
    return jax.shard_map(body, mesh=mesh, in_specs=in_specs, out_specs=out_specs, check_vma=False)
```
